32 devices in a mesh: dom: 16 (over z, x, core), rep: 2 (over y).
Axes of the slice: x: 2, y: 2, z: 4, core: 2. Of those that a mesh axis runs over, the one named last changes fastest.
Arguments:
- features: bfloat16 [131072, 128], P('dom'), may hold values from -6 to 6
- partition_map: int32 [131072], replicated, may hold values from 0 to 131071, as said below
- seed_ids: int32 [2048], P(('dom', 'rep')), may hold values from 0 to 131071, as said below
- hop1_ids: int32 [2048, 15], P(('dom', 'rep')), may hold values from 0 to 131071, as said below
- hop2_ids: int32 [2048, 15, 10], P(('dom', 'rep')), may hold values from 0 to 131071, as said below
- labels: int32 [2048], P(('dom', 'rep')), may hold values from 0 to 171
- self_one: bfloat16 [128, 256], replicated, may hold values from -0.5 to 0.5
- neigh_one: bfloat16 [128, 256], replicated, may hold values from -0.5 to 0.5
- bias_one: float32 [256], replicated, may hold values from -3 to 3
- self_two: bfloat16 [256, 172], replicated, may hold values from -0.375 to 0.375
- neigh_two: bfloat16 [256, 172], replicated, may hold values from -0.375 to 0.375
- bias_two: float32 [172], replicated, may hold values from -2 to 112, as said below
Outputs:
- seed_loss: float32 [2048], P(('dom', 'rep'))
- grad_self_one: float32 [128, 256], replicated
- grad_neigh_one: float32 [128, 256], replicated
- grad_bias_one: float32 [256], replicated
- grad_self_two: float32 [256, 172], replicated
- grad_neigh_two: float32 [256, 172], replicated
- grad_bias_two: float32 [172], replicated
The draws below stay inside these ranges and needn't reach their ends.
Inputs may be any that keep to these rules, and one draw needn't show every extreme that they name: A permutation of 0 to 131071: node v is stored at position p = partition_map[v], in partition p // 8192, row p % 8192. Rows below 256 of each partition hold hub nodes. `seed_ids`: node ids. `hop1_ids`: node ids. `hop2_ids`: take one device's 64 seeds (an aligned block of seeds) with all their hop-1 and hop-2 ids, 10624 ids with repeats counted, and map them through partition_map: at most 2428 positions fall in any one partition, and at most 332 fall in rows 256 and above of any one partition. Every device reaches both bounds. `bias_two`: class biases.
All inputs are finite; a program needn't handle non-finite values.
Results may differ from the reference program's by a relative error of at most 0.003.
Values may be sent and summed in bfloat16 or wider, within the bound.
A program may use at most 128 MiB of HBM per device.

```python
import jax
import jax.numpy as jnp
from jax import lax

FEAT = 128
HID = 256
CLASSES = 172
FAN1 = 15
FAN2 = 10
HOT_DEV = 256
SEEDS_DEV = 64
NODE_DEV = 8192
TREE = 166
COLD_CAP = 332
LOW_HOT = 80
HIGH_HOT = 2096
HUBS = 2
NODES = 131072
SEEDS_ALL = 2048
N_DOM = 16
N_REP = 2


def sample_plan(key):
    folded = jax.random.fold_in(key, 4242)
    key_map, key_hub, key_dev = jax.random.split(folded, 3)
    part_map = jax.random.permutation(key_map, NODES).astype(jnp.int32)
    hub_order = jax.random.permutation(key_hub, N_DOM).astype(jnp.int32)
    total_rows = SEEDS_DEV * TREE
    cold_total = N_DOM * COLD_CAP
    hub_total = HUBS * HIGH_HOT

    def one_device(dev_key):
        key_cold, key_hot, key_mix = jax.random.split(dev_key, 3)
        row_index = jnp.arange(total_rows, dtype=jnp.int32)
        is_cold = row_index < cold_total
        cold_owner = jnp.minimum(row_index // COLD_CAP, N_DOM - 1)
        hot_index = jnp.maximum(row_index - cold_total, 0)
        owner_rank = jnp.where(hot_index < hub_total, hot_index // HIGH_HOT, HUBS + (hot_index - hub_total) // LOW_HOT)
        hot_owner = hub_order[jnp.clip(owner_rank, 0, N_DOM - 1)]
        owners = jnp.where(is_cold, cold_owner, hot_owner)
        cold_row = jax.random.randint(key_cold, (total_rows,), HOT_DEV, NODE_DEV, dtype=jnp.int32)
        hot_row = jax.random.randint(key_hot, (total_rows,), 0, HOT_DEV, dtype=jnp.int32)
        store_place = owners * NODE_DEV + jnp.where(is_cold, cold_row, hot_row)
        return store_place[jax.random.permutation(key_mix, total_rows)]
    places = jax.vmap(one_device)(jax.random.split(key_dev, N_DOM * N_REP))
    inverse = jnp.zeros((NODES,), jnp.int32).at[part_map].set(jnp.arange(NODES, dtype=jnp.int32))
    return (part_map, inverse[places])


def draw_partition_map(key, part):
    part_map, node_ids = sample_plan(key)
    return part_map


def draw_seed_ids(key, part):
    part_map, node_ids = sample_plan(key)
    return node_ids[:, :SEEDS_DEV].reshape(-1)


def draw_hop1_ids(key, part):
    part_map, node_ids = sample_plan(key)
    return node_ids[:, SEEDS_DEV:SEEDS_DEV * (1 + FAN1)].reshape(N_DOM * N_REP * SEEDS_DEV, FAN1)


def draw_hop2_ids(key, part):
    part_map, node_ids = sample_plan(key)
    return node_ids[:, SEEDS_DEV * (1 + FAN1):].reshape(N_DOM * N_REP * SEEDS_DEV, FAN1, FAN2)


def draw_bias_two(key, part):
    centred = 0.5 * jax.random.truncated_normal(key, -4.0, 4.0, (CLASSES,), jnp.float32)
    return centred


def set_ends(result, key, low, high):
    shape = result.shape
    index_at = [jax.random.randint(jax.random.fold_in(key, axis), (), 0, shape[axis]) for axis in range(len(shape))]
    result = result.at[tuple(index_at)].set(low)
    longest = shape.index(max(shape))
    index_at[longest] = (index_at[longest] + 1) % shape[longest]
    return result.at[tuple(index_at)].set(high)


def shard_levels(stream_key, dims, cuts, smallest, largest):
    loudness = 1.0
    for axis_at, parts in cuts:
        heights = jax.random.uniform(jax.random.fold_in(jax.random.fold_in(stream_key, 6), axis_at), (parts,), jnp.float32, smallest / len(cuts), largest / len(cuts))
        loudness = loudness * jnp.repeat(jnp.exp(heights), dims[axis_at] // parts).reshape((-1,) + (1,) * (len(dims) - 1 - axis_at))
    return loudness


def noise(stream_key, dims, scale, reach, cuts=(), kind=jnp.bfloat16):
    drawn = scale * jax.random.normal(stream_key, dims, jnp.float32)
    if cuts:
        drawn = drawn * shard_levels(stream_key, dims, cuts, -0.22, 0.18)
    return jnp.clip(drawn, -reach, reach).astype(kind)


def setup_inputs(seed: int = 0) -> dict:
    key_list = jax.random.split(jax.random.key(seed), 13)
    features = noise(key_list[0], (NODES, FEAT), 1.0, 6.0, ((0, 16),))
    partition_map = draw_partition_map(jax.random.fold_in(key_list[12], 71), 0)
    seed_ids = draw_seed_ids(jax.random.fold_in(key_list[12], 71), 0)
    hop1_ids = draw_hop1_ids(jax.random.fold_in(key_list[12], 71), 0)
    hop2_ids = draw_hop2_ids(jax.random.fold_in(key_list[12], 71), 0)
    labels = set_ends(jax.random.randint(key_list[5], (SEEDS_ALL,), 0, CLASSES), jax.random.fold_in(key_list[5], 1), 0, CLASSES - 1).astype(jnp.int32)
    self_one = noise(key_list[6], (FEAT, HID), FEAT ** -0.5, 0.5)
    neigh_one = noise(key_list[7], (FEAT, HID), FEAT ** -0.5, 0.5)
    bias_one = noise(key_list[8], (HID,), 0.5, 3.0, (), jnp.float32)
    self_two = noise(key_list[9], (HID, CLASSES), HID ** -0.5, 0.375)
    neigh_two = noise(key_list[10], (HID, CLASSES), HID ** -0.5, 0.375)
    bias_two = draw_bias_two(jax.random.fold_in(key_list[12], 71), 0)
    return {"features": features, "partition_map": partition_map, "seed_ids": seed_ids, "hop1_ids": hop1_ids, "hop2_ids": hop2_ids, "labels": labels, "self_one": self_one, "neigh_one": neigh_one, "bias_one": bias_one, "self_two": self_two, "neigh_two": neigh_two, "bias_two": bias_two}


def activate(values):
    return jax.nn.gelu(values, approximate=True)

def sage_terms(seed_rows, hop_rows, far_rows, labels, self_one, neigh_one, bias_one, self_two, neigh_two, bias_two):
    seed_count = seed_rows.shape[0]
    fan_one = hop_rows.shape[0] // seed_count
    feat_width = seed_rows.shape[1]
    hidden = self_one.shape[1]
    seed_mean = lax.optimization_barrier(jnp.mean(hop_rows.reshape(seed_count, fan_one, feat_width), axis=1, dtype=jnp.float32)).astype(jnp.bfloat16)
    far_mean = lax.optimization_barrier(jnp.mean(far_rows, axis=1, dtype=jnp.float32)).astype(jnp.bfloat16)
    pre_seed = jnp.dot(seed_rows, self_one, preferred_element_type=jnp.float32) + jnp.dot(seed_mean, neigh_one, preferred_element_type=jnp.float32) + bias_one
    pre_hop = jnp.dot(hop_rows, self_one, preferred_element_type=jnp.float32) + jnp.dot(far_mean, neigh_one, preferred_element_type=jnp.float32) + bias_one
    act_seed, back_seed = jax.vjp(activate, pre_seed)
    act_hop, back_hop = jax.vjp(activate, pre_hop)
    hid_seed = act_seed.astype(jnp.bfloat16)
    hid_hop = act_hop.astype(jnp.bfloat16)
    hop_mean = lax.optimization_barrier(jnp.mean(hid_hop.reshape(seed_count, fan_one, hidden), axis=1, dtype=jnp.float32)).astype(jnp.bfloat16)
    logits = jnp.dot(hid_seed, self_two, preferred_element_type=jnp.float32) + jnp.dot(hop_mean, neigh_two, preferred_element_type=jnp.float32) + bias_two
    peak_value = lax.optimization_barrier(jnp.max(logits, axis=1, keepdims=True))
    shifted = logits - peak_value
    log_total = jnp.log(lax.optimization_barrier(jnp.sum(jnp.exp(shifted), axis=1, keepdims=True)))
    log_probs = shifted - log_total
    class_iota = lax.broadcasted_iota(jnp.int32, logits.shape, 1)
    target = (labels[:, None] == class_iota).astype(jnp.float32)
    seed_loss = -lax.optimization_barrier(jnp.sum(log_probs * target, axis=1))
    d_logits = ((jnp.exp(log_probs) - target) / seed_count).astype(jnp.bfloat16)
    grad_self_two = jnp.dot(hid_seed.T, d_logits, preferred_element_type=jnp.float32)
    grad_neigh_two = jnp.dot(hop_mean.T, d_logits, preferred_element_type=jnp.float32)
    grad_bias_two = lax.optimization_barrier(jnp.sum(d_logits.astype(jnp.float32), axis=0))
    d_hid_seed = jnp.dot(d_logits, self_two.T, preferred_element_type=jnp.float32)
    d_hop_mean = jnp.dot(d_logits, neigh_two.T, preferred_element_type=jnp.float32)
    d_pre_seed = back_seed(d_hid_seed)[0].astype(jnp.bfloat16)
    spread = jnp.broadcast_to((d_hop_mean / fan_one)[:, None, :], (seed_count, fan_one, hidden)).reshape(seed_count * fan_one, hidden)
    d_pre_hop = back_hop(spread)[0].astype(jnp.bfloat16)
    grad_self_one = jnp.dot(seed_rows.T, d_pre_seed, preferred_element_type=jnp.float32) + jnp.dot(hop_rows.T, d_pre_hop, preferred_element_type=jnp.float32)
    grad_neigh_one = jnp.dot(seed_mean.T, d_pre_seed, preferred_element_type=jnp.float32) + jnp.dot(far_mean.T, d_pre_hop, preferred_element_type=jnp.float32)
    grad_bias_one = lax.optimization_barrier(jnp.sum(d_pre_seed.astype(jnp.float32), axis=0)) + lax.optimization_barrier(jnp.sum(d_pre_hop.astype(jnp.float32), axis=0))
    return (seed_loss, (grad_self_one, grad_neigh_one, grad_bias_one, grad_self_two, grad_neigh_two, grad_bias_two))

def reference(features, partition_map, seed_ids, hop1_ids, hop2_ids, labels, self_one, neigh_one, bias_one, self_two, neigh_two, bias_two):
    devices = N_DOM * N_REP
    seed_blocks = seed_ids.reshape(devices, SEEDS_DEV)
    hop_blocks = hop1_ids.reshape(devices, SEEDS_DEV * FAN1)
    far_blocks = hop2_ids.reshape(devices, SEEDS_DEV * FAN1, FAN2)
    label_blocks = labels.reshape(devices, SEEDS_DEV)
    initial = (jnp.zeros((FEAT, HID), jnp.float32), jnp.zeros((FEAT, HID), jnp.float32), jnp.zeros((HID,), jnp.float32), jnp.zeros((HID, CLASSES), jnp.float32), jnp.zeros((HID, CLASSES), jnp.float32), jnp.zeros((CLASSES,), jnp.float32))

    def one_block(totals, pieces):
        seeds_here, hops_here, far_here, labels_here = pieces
        seed_rows = features[partition_map[seeds_here]]
        hop_rows = features[partition_map[hops_here]]
        far_rows = features[partition_map[far_here]]
        seed_loss, grads = sage_terms(seed_rows, hop_rows, far_rows, labels_here, self_one, neigh_one, bias_one, self_two, neigh_two, bias_two)
        return (jax.tree.map(jnp.add, totals, grads), seed_loss)
    totals, losses = lax.scan(one_block, initial, (seed_blocks, hop_blocks, far_blocks, label_blocks))
    return (losses.reshape(-1), totals[0], totals[1], totals[2], totals[3], totals[4], totals[5])
```

```python
import functools

import jax
import jax.numpy as jnp
from jax import lax
from jax.experimental import pallas as pl
from jax.experimental.pallas import tpu as pltpu
from jax.sharding import PartitionSpec as P

HOT_DEV = 256
LANES = 128
MESH = pl.DeviceIdType.MESH
VMEM_LIMIT = 56 * 1024 * 1024


def round_up(value, unit):
    return -(-value // unit) * unit


def dot_tn(left, right):
    return lax.dot_general(left, right, (((0,), (0,)), ((), ())), preferred_element_type=jnp.float32)


def dot_nt(left, right):
    return lax.dot_general(left, right, (((1,), (1,)), ((), ())), preferred_element_type=jnp.float32)


def dot_nn(left, right):
    return jnp.dot(left, right, preferred_element_type=jnp.float32)


def plan_kernel(ids_ref, map_ref, req_ref, addr_ref, own_ref, slot_ref, val_ref, *, parts, shift, stride, id_rows, cap_pad):
    rows = ids_ref.shape[0]
    blocks = rows // 8
    tiles = [ids_ref[8 * v : 8 * v + 8, :] for v in range(blocks)]
    high = [tile >> 7 for tile in tiles]
    low = [tile & (LANES - 1) for tile in tiles]

    def lookup(step, found):
        base = pl.multiple_of(step * 8, 8)
        block = map_ref[pl.ds(base, 8), :]
        found = list(found)
        for k in range(8):
            row = jnp.broadcast_to(block[k : k + 1, :], (8, LANES))
            for v in range(blocks):
                got = jnp.take_along_axis(row, low[v], axis=1, mode="promise_in_bounds")
                found[v] = jnp.where(high[v] == base + k, got, found[v])
        return tuple(found)

    zero = jnp.zeros((8, LANES), jnp.int32)
    found = lax.fori_loop(0, map_ref.shape[0] // 8, lookup, (zero,) * blocks)
    position = jnp.concatenate(found, axis=0)
    owner = position >> shift
    local = position & ((1 << shift) - 1)
    row_iota = lax.broadcasted_iota(jnp.int32, (rows, LANES), 0)
    is_cold = (local >= HOT_DEV) & (row_iota < id_rows)
    owner_cold = jnp.where(is_cold, owner, -1)
    upper = (
        lax.broadcasted_iota(jnp.int32, (LANES, LANES), 0) <= lax.broadcasted_iota(jnp.int32, (LANES, LANES), 1)
    ).astype(jnp.bfloat16)
    ones = jnp.ones((LANES, LANES), jnp.bfloat16)
    below = (
        lax.broadcasted_iota(jnp.int32, (rows, rows), 1) < lax.broadcasted_iota(jnp.int32, (rows, rows), 0)
    ).astype(jnp.bfloat16)
    slot = jnp.full((rows, LANES), -1.0, jnp.float32)
    for part in range(parts):
        hit = owner_cold == part
        member = hit.astype(jnp.bfloat16)
        ahead = dot_nn(below, member).astype(jnp.bfloat16)
        running = dot_nn(member, upper) + dot_nn(ahead, ones)
        slot = jnp.where(hit, running - 1.0, slot)
    slot = slot.astype(jnp.int32)
    addr_ref[...] = owner * stride + jnp.where(is_cold, HOT_DEV + slot, local)
    own_ref[...] = owner_cold
    slot_ref[...] = slot
    val_ref[...] = local
    part_iota = lax.broadcasted_iota(jnp.int32, (parts, LANES), 0)
    slot_iota = lax.broadcasted_iota(jnp.int32, (cap_pad, LANES), 0)

    def place(step, table):
        base = pl.multiple_of(step * 8, 8)
        own8 = own_ref[pl.ds(base, 8), :]
        slot8 = slot_ref[pl.ds(base, 8), :]
        val8 = val_ref[pl.ds(base, 8), :]
        for k in range(0, 8, 2):
            lefts, rights = [], []
            for q in range(k, k + 2):
                val = val8[q : q + 1, :].astype(jnp.float32)
                top = jnp.floor(val * (1.0 / LANES))
                mine = part_iota == own8[q : q + 1, :]
                lefts.append(
                    jnp.concatenate(
                        [jnp.where(mine, top, 0.0), jnp.where(mine, val - top * LANES, 0.0)], axis=0
                    ).astype(jnp.bfloat16)
                )
                rights.append((slot_iota == slot8[q : q + 1, :]).astype(jnp.bfloat16))
            table = table + dot_nt(jnp.concatenate(lefts, axis=1), jnp.concatenate(rights, axis=1))
        return table

    table = lax.fori_loop(0, blocks, place, jnp.zeros((2 * parts, cap_pad), jnp.float32))
    req_ref[...] = (table[:parts] * LANES + table[parts:]).astype(jnp.int32)


def plan(ids, partition_map, parts, node_rows, stride, id_rows, cap_pad):
    rows = ids.shape[0]
    kernel = functools.partial(
        plan_kernel,
        parts=parts,
        shift=node_rows.bit_length() - 1,
        stride=stride,
        id_rows=id_rows,
        cap_pad=cap_pad,
    )
    return pl.pallas_call(
        kernel,
        name="plan",
        out_shape=(
            jax.ShapeDtypeStruct((parts, cap_pad), jnp.int32),
            jax.ShapeDtypeStruct((rows, LANES), jnp.int32),
        ),
        in_specs=[pl.BlockSpec(memory_space=pltpu.VMEM)] * 2,
        out_specs=(pl.BlockSpec(memory_space=pltpu.VMEM),) * 2,
        scratch_shapes=[pltpu.VMEM((rows, LANES), jnp.int32)] * 3,
        compiler_params=pltpu.CompilerParams(vmem_limit_bytes=VMEM_LIMIT),
        cost_estimate=pl.CostEstimate(flops=40_000_000, bytes_accessed=1_000_000, transcendentals=0),
    )(ids, partition_map.reshape(-1, LANES))


ROOT = 0.7978845608028654
CUBE = 0.044715


def gelu_pair(pre):
    square = pre * pre
    bend = jnp.tanh(ROOT * pre * (1.0 + CUBE * square))
    half = 0.5 * (1.0 + bend)
    slope = half + 0.5 * pre * (1.0 - bend * bend) * (ROOT * (1.0 + 3.0 * CUBE * square))
    return pre * half, slope


def tree_sum(values):
    while len(values) > 1:
        values = [a + b for a, b in zip(values[::2], values[1::2])] + (
            [values[-1]] if len(values) % 2 else []
        )
    return values[0]


def model_kernel(
    addr_ref, table_ref, label_ref, w_one_ref, b_one_ref, w_two_ref, b_two_ref,
    loss_ref, g_one_ref, gb_one_ref, g_two_ref, gb_two_ref,
    wide, x_buf, far_buf, own_buf, slope_buf, d_buf, *, seeds, fan_one, fan_two,
):
    feat = table_ref.shape[1]
    hidden = w_one_ref.shape[1]
    hops = seeds * fan_one
    chunk = 64 if table_ref.shape[0] % 64 == 0 else 16

    def widen(step, carry):
        at = pl.ds(pl.multiple_of(step * chunk, chunk), chunk)
        wide[at, :] = table_ref[at, :].astype(jnp.float32)
        return carry

    lax.fori_loop(0, table_ref.shape[0] // chunk, widen, 0)

    def fetch(step, carry):
        j = step // (seeds // 8)
        block = step % (seeds // 8)
        base = pl.multiple_of(step * 8, 8)
        for k in range(8):
            hop = (block * 8 + k) * fan_one + j
            own_buf[pl.ds(base + k, 1), :] = wide[pl.ds(addr_ref[seeds + hop], 1), :]
            first = seeds + hops + hop * fan_two
            rows = [wide[pl.ds(addr_ref[first + m], 1), :] for m in range(fan_two)]
            far_buf[pl.ds(base + k, 1), :] = tree_sum(rows)
        return carry

    lax.fori_loop(0, hops // 8, fetch, 0)

    def fetch_seed(step, carry):
        base = pl.multiple_of(step * 8, 8)
        for k in range(8):
            own_buf[pl.ds(hops + base + k, 1), :] = wide[pl.ds(addr_ref[base + k], 1), :]
        return carry

    lax.fori_loop(0, seeds // 8, fetch_seed, 0)

    w_one = w_one_ref[...]
    b_one = b_one_ref[...]
    row_sum = jnp.zeros((seeds, feat), jnp.float32)
    hid_sum = jnp.zeros((seeds, hidden), jnp.float32)
    for j in range(fan_one):
        at = slice(j * seeds, (j + 1) * seeds)
        own = own_buf[at, :]
        row_sum = row_sum + own
        x_buf[at, :feat] = own.astype(jnp.bfloat16)
        x_buf[at, feat:] = (far_buf[at, :] * (1.0 / fan_two)).astype(jnp.bfloat16)
    x_buf[hops:, :feat] = own_buf[hops:, :].astype(jnp.bfloat16)
    x_buf[hops:, feat:] = (row_sum * (1.0 / fan_one)).astype(jnp.bfloat16)
    act = None
    for j in range(fan_one + 1):
        at = slice(j * seeds, (j + 1) * seeds)
        act, slope = gelu_pair(dot_nn(x_buf[at, :], w_one) + b_one)
        act = act.astype(jnp.bfloat16)
        slope_buf[at, :] = slope
        if j < fan_one:
            hid_sum = hid_sum + act.astype(jnp.float32)
    hid = jnp.concatenate([act, (hid_sum * (1.0 / fan_one)).astype(jnp.bfloat16)], axis=1)
    logits = dot_nn(hid, w_two_ref[...]) + b_two_ref[...]
    shifted = logits - jnp.max(logits, axis=1, keepdims=True)
    log_probs = shifted - jnp.log(jnp.sum(jnp.exp(shifted), axis=1, keepdims=True))
    class_iota = lax.broadcasted_iota(jnp.int32, logits.shape, 1)
    target = (class_iota == label_ref[...]).astype(jnp.float32)
    loss_ref[...] = -jnp.sum(log_probs * target, axis=1, keepdims=True)
    d_logits = ((jnp.exp(log_probs) - target) * (1.0 / seeds)).astype(jnp.bfloat16)
    g_two_ref[...] = dot_tn(hid, d_logits)
    gb_two_ref[...] = jnp.sum(d_logits.astype(jnp.float32), axis=0, keepdims=True)
    d_hid = dot_nt(d_logits, w_two_ref[...])
    d_hop = d_hid[:, hidden:] * (1.0 / fan_one)
    bias_sum = jnp.zeros((seeds, hidden), jnp.float32)
    for j in range(fan_one + 1):
        at = slice(j * seeds, (j + 1) * seeds)
        d_pre = ((d_hop if j < fan_one else d_hid[:, :hidden]) * slope_buf[at, :]).astype(jnp.bfloat16)
        d_buf[at, :] = d_pre
        bias_sum = bias_sum + d_pre.astype(jnp.float32)
    gb_one_ref[...] = jnp.sum(bias_sum, axis=0, keepdims=True)
    g_one_ref[...] = dot_tn(x_buf[...], d_buf[...])


def model(addr, table, labels, self_one, neigh_one, bias_one, self_two, neigh_two, bias_two, fan_one, fan_two):
    seeds = labels.shape[0]
    feat, hidden = self_one.shape
    classes = self_two.shape[1]
    total = seeds * (1 + fan_one)
    vmem = pl.BlockSpec(memory_space=pltpu.VMEM)
    return pl.pallas_call(
        functools.partial(model_kernel, seeds=seeds, fan_one=fan_one, fan_two=fan_two),
        name="model",
        out_shape=(
            jax.ShapeDtypeStruct((seeds, 1), jnp.float32),
            jax.ShapeDtypeStruct((2 * feat, hidden), jnp.float32),
            jax.ShapeDtypeStruct((1, hidden), jnp.float32),
            jax.ShapeDtypeStruct((2 * hidden, classes), jnp.float32),
            jax.ShapeDtypeStruct((1, classes), jnp.float32),
        ),
        in_specs=[pl.BlockSpec(memory_space=pltpu.SMEM)] + [vmem] * 6,
        out_specs=(vmem,) * 5,
        scratch_shapes=[
            pltpu.VMEM(table.shape, jnp.float32),
            pltpu.VMEM((total, 2 * feat), jnp.bfloat16),
            pltpu.VMEM((total - seeds, feat), jnp.float32),
            pltpu.VMEM((total, feat), jnp.float32),
            pltpu.VMEM((total, hidden), jnp.float32),
            pltpu.VMEM((total, hidden), jnp.bfloat16),
        ],
        compiler_params=pltpu.CompilerParams(vmem_limit_bytes=VMEM_LIMIT),
        cost_estimate=pl.CostEstimate(flops=100_000_000, bytes_accessed=4_000_000, transcendentals=0),
    )(
        addr,
        table,
        labels.reshape(seeds, 1),
        jnp.concatenate([self_one, neigh_one], axis=0),
        bias_one.reshape(1, hidden),
        jnp.concatenate([self_two, neigh_two], axis=0),
        bias_two.reshape(1, classes),
    )


def reduce_kernel(part_ref, out_ref, inbox, gathered, local_sem, send_sem, recv_sem, send_two, recv_two, *, n_dom, n_rep):
    count = n_dom * n_rep
    me = lax.axis_index("dom") * n_rep + lax.axis_index("rep")
    barrier = pltpu.get_barrier_semaphore()

    def peer(step):
        other = lax.rem(me + step, count)
        return other, {"dom": other // n_rep, "rep": lax.rem(other, n_rep)}

    def greet(step, carry):
        other, where = peer(step)
        pl.semaphore_signal(barrier, inc=1, device_id=where, device_id_type=MESH)
        return carry

    lax.fori_loop(1, count, greet, 0)
    keep = pltpu.make_async_copy(part_ref.at[me], inbox.at[me], local_sem)
    keep.start()
    pl.semaphore_wait(barrier, count - 1)

    def scatter(step, carry):
        other, where = peer(step)
        pltpu.make_async_remote_copy(
            part_ref.at[other], inbox.at[me], send_sem, recv_sem, device_id=where, device_id_type=MESH
        ).start()
        return carry

    lax.fori_loop(1, count, scatter, 0)
    keep.wait()
    most = pl.ds(0, count - 1)
    first = pltpu.make_async_remote_copy(
        part_ref.at[most], inbox.at[most], send_sem, recv_sem, device_id=peer(1)[1], device_id_type=MESH
    )
    first.wait_recv()
    total = inbox[0].astype(jnp.float32)

    def add(step, total):
        return total + inbox[step].astype(jnp.float32)

    total = lax.fori_loop(1, count, add, total)
    gathered[me] = total.astype(gathered.dtype)

    def spread(step, carry):
        other, where = peer(step)
        pltpu.make_async_remote_copy(
            gathered.at[me], gathered.at[me], send_two, recv_two, device_id=where, device_id_type=MESH
        ).start()
        return carry

    lax.fori_loop(1, count, spread, 0)
    second = pltpu.make_async_remote_copy(
        gathered.at[most], gathered.at[most], send_two, recv_two, device_id=peer(1)[1], device_id_type=MESH
    )
    second.wait_recv()
    first.wait_send()
    second.wait_send()
    out_ref[...] = gathered[...]


def sum_everywhere(pieces):
    n_dom, n_rep = lax.axis_size("dom"), lax.axis_size("rep")
    count = n_dom * n_rep
    vmem = pl.BlockSpec(memory_space=pltpu.VMEM)
    return pl.pallas_call(
        functools.partial(reduce_kernel, n_dom=n_dom, n_rep=n_rep),
        name="sum_everywhere",
        out_shape=jax.ShapeDtypeStruct(pieces.shape, pieces.dtype),
        in_specs=[vmem],
        out_specs=vmem,
        scratch_shapes=[
            pltpu.VMEM(pieces.shape, pieces.dtype),
            pltpu.VMEM(pieces.shape, pieces.dtype),
            pltpu.SemaphoreType.DMA,
            pltpu.SemaphoreType.DMA,
            pltpu.SemaphoreType.DMA,
            pltpu.SemaphoreType.DMA,
            pltpu.SemaphoreType.DMA,
        ],
        compiler_params=pltpu.CompilerParams(collective_id=1, has_side_effects=True, vmem_limit_bytes=VMEM_LIMIT),
    )(pieces)


def shards(
    features, partition_map, seed_ids, hop1_ids, hop2_ids, labels,
    self_one, neigh_one, bias_one, self_two, neigh_two, bias_two,
):
    parts = lax.axis_size("dom")
    count = parts * lax.axis_size("rep")
    seeds = seed_ids.shape[0]
    fan_one = hop1_ids.shape[1]
    fan_two = hop2_ids.shape[2]
    node_rows, feat = features.shape
    tree_rows = 1 + fan_one + fan_one * fan_two
    cold_cap = tree_rows // 2 * (seeds // parts)
    cap_row = round_up(cold_cap, 16)
    cap_pad = round_up(cold_cap, LANES)
    stride = HOT_DEV + cap_row
    total = seeds * tree_rows
    id_rows = total // LANES
    wanted = jnp.concatenate([seed_ids, hop1_ids.reshape(-1), hop2_ids.reshape(-1)])
    ids = jnp.pad(wanted.reshape(id_rows, LANES), ((0, round_up(id_rows, 8) - id_rows), (0, 0)))
    request, addr = plan(ids, partition_map, parts, node_rows, stride, id_rows, cap_pad)
    arrived = lax.all_to_all(request[:, :cap_row], "dom", split_axis=0, concat_axis=0, tiled=True)
    returned = lax.all_to_all(features[arrived], "dom", split_axis=0, concat_axis=0, tiled=True)
    hubs = lax.all_gather(features[:HOT_DEV], "dom", axis=0)
    table = jnp.concatenate([hubs, returned], axis=1).reshape(parts * stride, feat)
    loss, g_one, gb_one, g_two, gb_two = model(
        addr.reshape(-1), table, labels, self_one, neigh_one, bias_one, self_two, neigh_two, bias_two,
        fan_one, fan_two,
    )
    hidden, classes = self_two.shape
    sizes = [g_one.size, g_two.size, gb_one.size, gb_two.size]
    flat = jnp.concatenate([g_one.reshape(-1), g_two.reshape(-1), gb_one.reshape(-1), gb_two.reshape(-1)])
    rows = round_up(-(-flat.size // (count * LANES)), 8)
    flat = jnp.pad(flat, (0, count * rows * LANES - flat.size))
    summed = sum_everywhere(flat.reshape(count, rows, LANES)).reshape(-1)
    cuts = [0]
    for size in sizes:
        cuts.append(cuts[-1] + size)
    one = summed[cuts[0] : cuts[1]].reshape(2, feat, hidden)
    two = summed[cuts[1] : cuts[2]].reshape(2, hidden, classes)
    return (
        loss.reshape(-1), one[0], one[1], summed[cuts[2] : cuts[3]],
        two[0], two[1], summed[cuts[3] : cuts[4]],
    )


def solution(mesh):
    return jax.shard_map(
        shards,
        mesh=mesh,
        in_specs=(
            P("dom", None),
            P(),
            P(("dom", "rep")),
            P(("dom", "rep"), None),
            P(("dom", "rep"), None, None),
            P(("dom", "rep")),
            P(),
            P(),
            P(),
            P(),
            P(),
            P(),
        ),
        out_specs=(P(("dom", "rep")), P(), P(), P(), P(), P(), P()),
        check_vma=False,
    )
```

```python
import functools

import jax
import jax.numpy as jnp
from jax import lax
from jax.experimental import pallas as pl
from jax.experimental.pallas import tpu as pltpu
from jax.sharding import PartitionSpec as P

HOT_DEV = 256
LANES = 128
MESH = pl.DeviceIdType.MESH
WIRE = jnp.bfloat16
VMEM_LIMIT = 56 * 1024 * 1024


def round_up(value, unit):
    return -(-value // unit) * unit


def dot_tn(left, right):
    return lax.dot_general(left, right, (((0,), (0,)), ((), ())), preferred_element_type=jnp.float32)


def dot_nt(left, right):
    return lax.dot_general(left, right, (((1,), (1,)), ((), ())), preferred_element_type=jnp.float32)


def dot_nn(left, right):
    return jnp.dot(left, right, preferred_element_type=jnp.float32)


def plan_kernel(ids_ref, map_ref, req_ref, addr_ref, own_ref, slot_ref, val_ref, pos_ref, *, parts, shift, stride, id_rows, cap_pad):
    rows = ids_ref.shape[0]
    blocks = rows // 8
    stored = map_ref[...]
    pieces = jnp.concatenate([stored >> 16, (stored >> 8) & 255, stored & 255], axis=1)
    pieces = pieces.astype(jnp.float32).astype(jnp.bfloat16)
    map_iota = lax.broadcasted_iota(jnp.int32, map_ref.shape, 0)
    lane_iota = lax.broadcasted_iota(jnp.int32, (LANES, 2 * LANES), 0)

    def lookup(step, carry):
        base = pl.multiple_of(step * 8, 8)
        tile = ids_ref[pl.ds(base, 8), :]
        high, low = tile >> 7, tile & (LANES - 1)
        for k in range(0, 8, 2):
            hot = [(map_iota == high[q : q + 1, :]).astype(jnp.bfloat16) for q in (k, k + 1)]
            found = dot_tn(pieces, jnp.concatenate(hot, axis=1))
            found = found[:LANES] * 65536.0 + found[LANES : 2 * LANES] * 256.0 + found[2 * LANES :]
            lane = jnp.concatenate([low[k : k + 1, :], low[k + 1 : k + 2, :]], axis=1)
            picked = jnp.sum(jnp.where(lane_iota == lane, found, 0.0), axis=0, keepdims=True)
            pos_ref[pl.ds(base + k, 1), :] = picked[:, :LANES].astype(jnp.int32)
            pos_ref[pl.ds(base + k + 1, 1), :] = picked[:, LANES:].astype(jnp.int32)
        return carry

    lax.fori_loop(0, blocks, lookup, 0)
    position = pos_ref[...]
    owner = position >> shift
    local = position & ((1 << shift) - 1)
    row_iota = lax.broadcasted_iota(jnp.int32, (rows, LANES), 0)
    is_cold = (local >= HOT_DEV) & (row_iota < id_rows)
    owner_cold = jnp.where(is_cold, owner, -1)
    upper = (
        lax.broadcasted_iota(jnp.int32, (LANES, LANES), 0) <= lax.broadcasted_iota(jnp.int32, (LANES, LANES), 1)
    ).astype(jnp.bfloat16)
    ones = jnp.ones((LANES, LANES), jnp.bfloat16)
    below = (
        lax.broadcasted_iota(jnp.int32, (rows, rows), 1) < lax.broadcasted_iota(jnp.int32, (rows, rows), 0)
    ).astype(jnp.bfloat16)
    slot = jnp.full((rows, LANES), -1.0, jnp.float32)
    for part in range(parts):
        hit = owner_cold == part
        member = hit.astype(jnp.bfloat16)
        ahead = dot_nn(below, member).astype(jnp.bfloat16)
        running = dot_nn(member, upper) + dot_nn(ahead, ones)
        slot = jnp.where(hit, running - 1.0, slot)
    slot = slot.astype(jnp.int32)
    addr_ref[...] = owner * stride + jnp.where(is_cold, HOT_DEV + slot, local)
    own_ref[...] = owner_cold
    slot_ref[...] = slot
    val_ref[...] = local
    part_iota = lax.broadcasted_iota(jnp.int32, (parts, LANES), 0)
    slot_iota = lax.broadcasted_iota(jnp.int32, (cap_pad, LANES), 0)

    def place(step, table):
        base = pl.multiple_of(step * 8, 8)
        own8 = own_ref[pl.ds(base, 8), :]
        slot8 = slot_ref[pl.ds(base, 8), :]
        val8 = val_ref[pl.ds(base, 8), :]
        for k in range(0, 8, 2):
            lefts, rights = [], []
            for q in range(k, k + 2):
                val = val8[q : q + 1, :].astype(jnp.float32)
                top = jnp.floor(val * (1.0 / LANES))
                mine = part_iota == own8[q : q + 1, :]
                lefts.append(
                    jnp.concatenate(
                        [jnp.where(mine, top, 0.0), jnp.where(mine, val - top * LANES, 0.0)], axis=0
                    ).astype(jnp.bfloat16)
                )
                rights.append((slot_iota == slot8[q : q + 1, :]).astype(jnp.bfloat16))
            table = table + dot_nt(jnp.concatenate(lefts, axis=1), jnp.concatenate(rights, axis=1))
        return table

    table = lax.fori_loop(0, blocks, place, jnp.zeros((2 * parts, cap_pad), jnp.float32))
    request = (table[:parts] * LANES + table[parts:]).astype(jnp.int32)
    req_ref[...] = jnp.zeros(req_ref.shape, jnp.int32)
    for c in range(cap_pad // LANES):
        req_ref[:, c, :] = request[:, c * LANES : (c + 1) * LANES]


def plan(ids, partition_map, parts, node_rows, stride, id_rows, cap_pad):
    rows = ids.shape[0]
    kernel = functools.partial(
        plan_kernel,
        parts=parts,
        shift=node_rows.bit_length() - 1,
        stride=stride,
        id_rows=id_rows,
        cap_pad=cap_pad,
    )
    return pl.pallas_call(
        kernel,
        name="plan",
        out_shape=(
            jax.ShapeDtypeStruct((parts, round_up(cap_pad // LANES, 8), LANES), jnp.int32),
            jax.ShapeDtypeStruct((rows, LANES), jnp.int32),
        ),
        in_specs=[pl.BlockSpec(memory_space=pltpu.VMEM)] * 2,
        out_specs=(pl.BlockSpec(memory_space=pltpu.VMEM),) * 2,
        scratch_shapes=[pltpu.VMEM((rows, LANES), jnp.int32)] * 4,
        compiler_params=pltpu.CompilerParams(vmem_limit_bytes=VMEM_LIMIT),
        cost_estimate=pl.CostEstimate(flops=40_000_000, bytes_accessed=1_000_000, transcendentals=0),
    )(ids, partition_map.reshape(-1, LANES))


ROOT = 0.7978845608028654
CUBE = 0.044715


def gelu_pair(pre):
    square = pre * pre
    bend = jnp.tanh(ROOT * pre * (1.0 + CUBE * square))
    half = 0.5 * (1.0 + bend)
    slope = half + 0.5 * pre * (1.0 - bend * bend) * (ROOT * (1.0 + 3.0 * CUBE * square))
    return pre * half, slope


def tree_sum(values):
    while len(values) > 1:
        values = [a + b for a, b in zip(values[::2], values[1::2])] + (
            [values[-1]] if len(values) % 2 else []
        )
    return values[0]


def model_kernel(
    addr_ref, table_ref, label_ref, w_one_ref, b_one_ref, w_two_ref, b_two_ref,
    loss_ref, pack_ref,
    wide, x_buf, far_buf, own_buf, slope_buf, d_buf, *, seeds, fan_one, fan_two,
):
    feat = table_ref.shape[1]
    hidden = w_one_ref.shape[1]
    hops = seeds * fan_one
    chunk = 64 if table_ref.shape[0] % 64 == 0 else 16

    def widen(step, carry):
        at = pl.ds(pl.multiple_of(step * chunk, chunk), chunk)
        wide[at, :] = table_ref[at, :].astype(jnp.float32)
        return carry

    lax.fori_loop(0, table_ref.shape[0] // chunk, widen, 0)

    def fetch(step, carry):
        j = step // (seeds // 8)
        block = step % (seeds // 8)
        base = pl.multiple_of(step * 8, 8)
        for k in range(8):
            hop = (block * 8 + k) * fan_one + j
            own_buf[pl.ds(base + k, 1), :] = wide[pl.ds(addr_ref[seeds + hop], 1), :]
            first = seeds + hops + hop * fan_two
            rows = [wide[pl.ds(addr_ref[first + m], 1), :] for m in range(fan_two)]
            far_buf[pl.ds(base + k, 1), :] = tree_sum(rows)
        return carry

    lax.fori_loop(0, hops // 8, fetch, 0)

    def fetch_seed(step, carry):
        base = pl.multiple_of(step * 8, 8)
        for k in range(8):
            own_buf[pl.ds(hops + base + k, 1), :] = wide[pl.ds(addr_ref[base + k], 1), :]
        return carry

    lax.fori_loop(0, seeds // 8, fetch_seed, 0)

    w_one = w_one_ref[...]
    b_one = b_one_ref[...]
    row_sum = jnp.zeros((seeds, feat), jnp.float32)
    hid_sum = jnp.zeros((seeds, hidden), jnp.float32)
    for j in range(fan_one):
        at = slice(j * seeds, (j + 1) * seeds)
        own = own_buf[at, :]
        row_sum = row_sum + own
        x_buf[at, :feat] = own.astype(jnp.bfloat16)
        x_buf[at, feat:] = (far_buf[at, :] * (1.0 / fan_two)).astype(jnp.bfloat16)
    x_buf[hops:, :feat] = own_buf[hops:, :].astype(jnp.bfloat16)
    x_buf[hops:, feat:] = (row_sum * (1.0 / fan_one)).astype(jnp.bfloat16)
    act = None
    for j in range(fan_one + 1):
        at = slice(j * seeds, (j + 1) * seeds)
        act, slope = gelu_pair(dot_nn(x_buf[at, :], w_one) + b_one)
        act = act.astype(jnp.bfloat16)
        slope_buf[at, :] = slope
        if j < fan_one:
            hid_sum = hid_sum + act.astype(jnp.float32)
    hid = jnp.concatenate([act, (hid_sum * (1.0 / fan_one)).astype(jnp.bfloat16)], axis=1)
    logits = dot_nn(hid, w_two_ref[...]) + b_two_ref[...]
    shifted = logits - jnp.max(logits, axis=1, keepdims=True)
    log_probs = shifted - jnp.log(jnp.sum(jnp.exp(shifted), axis=1, keepdims=True))
    class_iota = lax.broadcasted_iota(jnp.int32, logits.shape, 1)
    target = (class_iota == label_ref[...]).astype(jnp.float32)
    loss_ref[...] = -jnp.sum(log_probs * target, axis=1, keepdims=True)
    d_logits = ((jnp.exp(log_probs) - target) * (1.0 / seeds)).astype(jnp.bfloat16)
    g_two = dot_tn(hid, d_logits)
    gb_two = jnp.sum(d_logits.astype(jnp.float32), axis=0, keepdims=True)
    d_hid = dot_nt(d_logits, w_two_ref[...])
    d_hop = d_hid[:, hidden:] * (1.0 / fan_one)
    bias_sum = jnp.zeros((seeds, hidden), jnp.float32)
    for j in range(fan_one + 1):
        at = slice(j * seeds, (j + 1) * seeds)
        d_pre = ((d_hop if j < fan_one else d_hid[:, :hidden]) * slope_buf[at, :]).astype(jnp.bfloat16)
        d_buf[at, :] = d_pre
        bias_sum = bias_sum + d_pre.astype(jnp.float32)
    gb_one = jnp.sum(bias_sum, axis=0, keepdims=True)
    pack_gradients(pack_ref, dot_tn(x_buf[...], d_buf[...]), gb_one, g_two, gb_two)


def model(addr, table, labels, self_one, neigh_one, bias_one, self_two, neigh_two, bias_two, fan_one, fan_two, pack_rows):
    seeds = labels.shape[0]
    feat, hidden = self_one.shape
    classes = self_two.shape[1]
    total = seeds * (1 + fan_one)
    vmem = pl.BlockSpec(memory_space=pltpu.VMEM)
    return pl.pallas_call(
        functools.partial(model_kernel, seeds=seeds, fan_one=fan_one, fan_two=fan_two),
        name="model",
        out_shape=(
            jax.ShapeDtypeStruct((seeds, 1), jnp.float32),
            jax.ShapeDtypeStruct((pack_rows, LANES), WIRE),
        ),
        in_specs=[pl.BlockSpec(memory_space=pltpu.SMEM)] + [vmem] * 6,
        out_specs=(vmem,) * 2,
        scratch_shapes=[
            pltpu.VMEM(table.shape, jnp.float32),
            pltpu.VMEM((total, 2 * feat), jnp.bfloat16),
            pltpu.VMEM((total - seeds, feat), jnp.float32),
            pltpu.VMEM((total, feat), jnp.float32),
            pltpu.VMEM((total, hidden), jnp.float32),
            pltpu.VMEM((total, hidden), jnp.bfloat16),
        ],
        compiler_params=pltpu.CompilerParams(vmem_limit_bytes=VMEM_LIMIT),
        cost_estimate=pl.CostEstimate(flops=100_000_000, bytes_accessed=4_000_000, transcendentals=0),
    )(
        addr,
        table,
        labels.reshape(seeds, 1),
        jnp.concatenate([self_one, neigh_one], axis=0),
        bias_one.reshape(1, hidden),
        jnp.concatenate([self_two, neigh_two], axis=0),
        bias_two.reshape(1, classes),
    )


def exchange_kernel(
    req_ref, feat_ref, out_ref, inbox, wanted, wide, stage, send,
    local_sem, req_send, req_recv, hub_send, hub_recv, row_send, row_recv, *, parts,
):
    node_rows = feat_ref.shape[0]
    cap_row = send.shape[1]
    me = lax.axis_index("dom")
    barrier = pltpu.get_barrier_semaphore()

    def where(step):
        other = lax.rem(me + step, parts)
        return other, {"dom": other}

    def greet(step, carry):
        pl.semaphore_signal(barrier, inc=1, device_id=where(step)[1], device_id_type=MESH)
        return carry

    lax.fori_loop(1, parts, greet, 0)
    keep_req = pltpu.make_async_copy(req_ref.at[me], inbox.at[me], local_sem.at[0])
    keep_req.start()
    keep_hub = pltpu.make_async_copy(feat_ref.at[pl.ds(0, HOT_DEV)], out_ref.at[me, pl.ds(0, HOT_DEV)], local_sem.at[1])
    keep_hub.start()
    pl.semaphore_wait(barrier, parts - 1)

    def ask(step, carry):
        other, at = where(step)
        pltpu.make_async_remote_copy(
            req_ref.at[other], inbox.at[me], req_send, req_recv, device_id=at, device_id_type=MESH
        ).start()
        return carry

    def share(step, carry):
        pltpu.make_async_remote_copy(
            feat_ref.at[pl.ds(0, HOT_DEV)], out_ref.at[me, pl.ds(0, HOT_DEV)], hub_send, hub_recv,
            device_id=where(step)[1], device_id_type=MESH,
        ).start()
        return carry

    lax.fori_loop(1, parts, ask, 0)
    lax.fori_loop(1, parts, share, 0)

    def widen(step, carry):
        at = pl.ds(pl.multiple_of(step * 64, 64), 64)
        wide[at, :] = feat_ref[at, :].astype(jnp.float32)
        return carry

    lax.fori_loop(0, node_rows // 64, widen, 0)
    most = pl.ds(0, parts - 1)
    asked = pltpu.make_async_remote_copy(
        req_ref.at[most], inbox.at[most], req_send, req_recv, device_id=where(1)[1], device_id_type=MESH
    )
    keep_req.wait()
    asked.wait_recv()
    to_scalar = pltpu.make_async_copy(inbox, wanted, local_sem.at[2])
    to_scalar.start()
    to_scalar.wait()

    def collect(other):
        def block(step, carry):
            base = pl.multiple_of(step * 16, 16)
            row = step // (LANES // 16)
            lane = lax.rem(step, LANES // 16) * 16
            for k in range(16):
                stage[pl.ds(base + k, 1), :] = wide[pl.ds(wanted[other, row, lane + k], 1), :]
            return carry

        lax.fori_loop(0, cap_row // 16, block, 0)
        return stage[...].astype(jnp.bfloat16)

    rows_at = pl.ds(HOT_DEV, cap_row)

    def serve(step, carry):
        other, at = where(step)
        send[other] = collect(other)
        pltpu.make_async_remote_copy(
            send.at[other], out_ref.at[me, rows_at], row_send, row_recv, device_id=at, device_id_type=MESH
        ).start()
        return carry

    lax.fori_loop(1, parts, serve, 0)
    out_ref[me, HOT_DEV:, :] = collect(me)
    hubs = pltpu.make_async_remote_copy(
        out_ref.at[most, pl.ds(0, HOT_DEV)], out_ref.at[most, pl.ds(0, HOT_DEV)], hub_send, hub_recv,
        device_id=where(1)[1], device_id_type=MESH,
    )
    rows = pltpu.make_async_remote_copy(
        send.at[most], out_ref.at[most, rows_at], row_send, row_recv, device_id=where(1)[1], device_id_type=MESH
    )
    keep_hub.wait()
    asked.wait_send()
    hubs.wait()
    rows.wait()


def exchange(request, features, cap_row):
    parts = lax.axis_size("dom")
    node_rows, feat = features.shape
    vmem = pl.BlockSpec(memory_space=pltpu.VMEM)
    return pl.pallas_call(
        functools.partial(exchange_kernel, parts=parts),
        name="exchange",
        out_shape=jax.ShapeDtypeStruct((parts, HOT_DEV + cap_row, feat), features.dtype),
        in_specs=[vmem, vmem],
        out_specs=vmem,
        scratch_shapes=[
            pltpu.VMEM(request.shape, jnp.int32),
            pltpu.SMEM(request.shape, jnp.int32),
            pltpu.VMEM((node_rows, feat), jnp.float32),
            pltpu.VMEM((cap_row, feat), jnp.float32),
            pltpu.VMEM((parts, cap_row, feat), features.dtype),
            pltpu.SemaphoreType.DMA((3,)),
        ]
        + [pltpu.SemaphoreType.DMA] * 6,
        compiler_params=pltpu.CompilerParams(collective_id=2, has_side_effects=True, vmem_limit_bytes=VMEM_LIMIT),
    )(request, features)


def pack_plan(feat, hidden, classes):
    halves = hidden // LANES
    one = 2 * feat * halves
    low = one + 2 * hidden
    tail = low + hidden
    return halves, one, low, tail, tail + 16


def pack_gradients(pack_ref, g_one, gb_one, g_two, gb_two):
    hidden, feat = g_one.shape[1], g_one.shape[0] // 2
    classes = g_two.shape[1]
    halves, one, low, tail, used = pack_plan(feat, hidden, classes)
    kind = pack_ref.dtype
    for h in range(halves):
        pack_ref[h * 2 * feat : (h + 1) * 2 * feat, :] = g_one[:, h * LANES : (h + 1) * LANES].astype(kind)
    pack_ref[one:low, :] = g_two[:, :LANES].astype(kind)
    rest = classes - LANES
    blank = jnp.zeros((hidden, LANES // 2 - rest), jnp.float32)
    high = jnp.concatenate([g_two[:hidden, LANES:], blank, g_two[hidden:, LANES:], blank], axis=1)
    pack_ref[low:tail, :] = high.astype(kind)
    wide = jnp.concatenate([gb_two, jnp.zeros((1, 2 * LANES - classes), jnp.float32)], axis=1)
    pieces = [gb_one[:, h * LANES : (h + 1) * LANES] for h in range(halves)]
    pieces += [wide[:, :LANES], wide[:, LANES:], jnp.zeros((16 - halves - 2, LANES), jnp.float32)]
    pack_ref[tail:used, :] = jnp.concatenate(pieces, axis=0).astype(kind)
    if pack_ref.shape[0] > used:
        pack_ref[used:, :] = jnp.zeros((pack_ref.shape[0] - used, LANES), kind)


def reduce_kernel(
    part_ref, self_one, neigh_one, bias_one, self_two, neigh_two, bias_two,
    inbox, gathered, local_sem, send_sem, recv_sem, send_two, recv_two, *, n_dom, n_rep,
):
    count = n_dom * n_rep
    rows = part_ref.shape[0] // count
    me = lax.axis_index("dom") * n_rep + lax.axis_index("rep")
    barrier = pltpu.get_barrier_semaphore()

    def peer(step):
        other = lax.rem(me + step, count)
        return other, {"dom": other // n_rep, "rep": lax.rem(other, n_rep)}

    def block(index):
        return pl.ds(pl.multiple_of(index * rows, rows), rows)

    def greet(step, carry):
        pl.semaphore_signal(barrier, inc=1, device_id=peer(step)[1], device_id_type=MESH)
        return carry

    lax.fori_loop(1, count, greet, 0)
    keep = pltpu.make_async_copy(part_ref.at[block(me)], inbox.at[block(me)], local_sem)
    keep.start()
    pl.semaphore_wait(barrier, count - 1)

    def scatter(step, carry):
        other, where = peer(step)
        pltpu.make_async_remote_copy(
            part_ref.at[block(other)], inbox.at[block(me)], send_sem, recv_sem, device_id=where, device_id_type=MESH
        ).start()
        return carry

    lax.fori_loop(1, count, scatter, 0)
    keep.wait()
    most = pl.ds(0, (count - 1) * rows)
    first = pltpu.make_async_remote_copy(
        part_ref.at[most], inbox.at[most], send_sem, recv_sem, device_id=peer(1)[1], device_id_type=MESH
    )
    first.wait_recv()

    def add(step, total):
        return total + inbox[block(step), :].astype(jnp.float32)

    total = lax.fori_loop(0, count, add, jnp.zeros((rows, LANES), jnp.float32))
    gathered[block(me), :] = total.astype(gathered.dtype)

    def spread(step, carry):
        pltpu.make_async_remote_copy(
            gathered.at[block(me)], gathered.at[block(me)], send_two, recv_two,
            device_id=peer(step)[1], device_id_type=MESH,
        ).start()
        return carry

    lax.fori_loop(1, count, spread, 0)
    second = pltpu.make_async_remote_copy(
        gathered.at[most], gathered.at[most], send_two, recv_two, device_id=peer(1)[1], device_id_type=MESH
    )
    second.wait_recv()
    first.wait_send()
    second.wait_send()
    feat, hidden = self_one.shape
    classes = self_two.shape[1]
    rest = classes - LANES
    halves, one, low, tail, used = pack_plan(feat, hidden, classes)
    for h in range(halves):
        cols = slice(h * LANES, (h + 1) * LANES)
        at = h * 2 * feat
        self_one[:, cols] = gathered[at : at + feat, :].astype(jnp.float32)
        neigh_one[:, cols] = gathered[at + feat : at + 2 * feat, :].astype(jnp.float32)
    self_two[:, :LANES] = gathered[one : one + hidden, :].astype(jnp.float32)
    neigh_two[:, :LANES] = gathered[one + hidden : low, :].astype(jnp.float32)
    high = gathered[low:tail, :].astype(jnp.float32)
    self_two[:, LANES:] = high[:, :rest]
    neigh_two[:, LANES:] = high[:, LANES // 2 : LANES // 2 + rest]
    last = gathered[tail:used, :].astype(jnp.float32)
    for h in range(halves):
        bias_one[:, h * LANES : (h + 1) * LANES] = last[h : h + 1, :]
    bias_two[:, :LANES] = last[halves : halves + 1, :]
    bias_two[:, LANES:] = last[halves + 1 : halves + 2, :rest]


def sum_everywhere(pieces, feat, hidden, classes):
    n_dom, n_rep = lax.axis_size("dom"), lax.axis_size("rep")
    vmem = pl.BlockSpec(memory_space=pltpu.VMEM)
    shapes = [(feat, hidden), (feat, hidden), (1, hidden), (hidden, classes), (hidden, classes), (1, classes)]
    return pl.pallas_call(
        functools.partial(reduce_kernel, n_dom=n_dom, n_rep=n_rep),
        name="sum_everywhere",
        out_shape=tuple(jax.ShapeDtypeStruct(shape, jnp.float32) for shape in shapes),
        in_specs=[vmem],
        out_specs=(vmem,) * 6,
        scratch_shapes=[pltpu.VMEM(pieces.shape, pieces.dtype)] * 2 + [pltpu.SemaphoreType.DMA] * 5,
        compiler_params=pltpu.CompilerParams(collective_id=1, has_side_effects=True, vmem_limit_bytes=VMEM_LIMIT),
    )(pieces)


def shards(
    features, partition_map, seed_ids, hop1_ids, hop2_ids, labels,
    self_one, neigh_one, bias_one, self_two, neigh_two, bias_two,
):
    parts = lax.axis_size("dom")
    count = parts * lax.axis_size("rep")
    seeds = seed_ids.shape[0]
    fan_one = hop1_ids.shape[1]
    fan_two = hop2_ids.shape[2]
    node_rows, feat = features.shape
    tree_rows = 1 + fan_one + fan_one * fan_two
    cold_cap = tree_rows // 2 * (seeds // parts)
    cap_row = round_up(cold_cap, 16)
    cap_pad = round_up(cold_cap, LANES)
    stride = HOT_DEV + cap_row
    total = seeds * tree_rows
    id_rows = total // LANES
    wanted = jnp.concatenate([seed_ids, hop1_ids.reshape(-1), hop2_ids.reshape(-1)])
    ids = jnp.pad(wanted.reshape(id_rows, LANES), ((0, round_up(id_rows, 8) - id_rows), (0, 0)))
    request, addr = plan(ids, partition_map, parts, node_rows, stride, id_rows, cap_pad)
    table = exchange(request, features, cap_row).reshape(parts * stride, feat)
    hidden, classes = self_two.shape
    used = pack_plan(feat, hidden, classes)[-1]
    pack_rows = count * round_up(-(-used // count), 16)
    loss, pieces = model(
        addr.reshape(-1), table, labels, self_one, neigh_one, bias_one, self_two, neigh_two, bias_two,
        fan_one, fan_two, pack_rows,
    )
    grads = sum_everywhere(pieces, feat, hidden, classes)
    return (
        loss.reshape(-1), grads[0], grads[1], grads[2].reshape(-1),
        grads[3], grads[4], grads[5].reshape(-1),
    )


def solution(mesh):
    return jax.shard_map(
        shards,
        mesh=mesh,
        in_specs=(
            P("dom", None),
            P(),
            P(("dom", "rep")),
            P(("dom", "rep"), None),
            P(("dom", "rep"), None, None),
            P(("dom", "rep")),
            P(),
            P(),
            P(),
            P(),
            P(),
            P(),
        ),
        out_specs=(P(("dom", "rep")), P(), P(), P(), P(), P(), P()),
        check_vma=False,
    )
```

```python
import functools

import jax
import jax.numpy as jnp
from jax import lax
from jax.experimental import pallas as pl
from jax.experimental.pallas import tpu as pltpu
from jax.sharding import PartitionSpec as P

HOT_DEV = 256
LANES = 128
MESH = pl.DeviceIdType.MESH
VMEM_LIMIT = 56 * 1024 * 1024


def round_up(value, unit):
    return -(-value // unit) * unit


def dot_tn(left, right):
    return lax.dot_general(left, right, (((0,), (0,)), ((), ())), preferred_element_type=jnp.float32)


def dot_nt(left, right):
    return lax.dot_general(left, right, (((1,), (1,)), ((), ())), preferred_element_type=jnp.float32)


def dot_nn(left, right):
    return jnp.dot(left, right, preferred_element_type=jnp.float32)


def plan_kernel(ids_ref, map_ref, req_ref, addr_ref, own_ref, slot_ref, val_ref, pos_ref, *, parts, shift, stride, id_rows, cap_pad):
    rows = ids_ref.shape[0]
    blocks = rows // 8
    stored = map_ref[...]
    pieces = jnp.concatenate([stored >> 16, (stored >> 8) & 255, stored & 255], axis=1)
    pieces = pieces.astype(jnp.float32).astype(jnp.bfloat16)
    map_iota = lax.broadcasted_iota(jnp.int32, map_ref.shape, 0)
    lane_iota = lax.broadcasted_iota(jnp.int32, (LANES, 2 * LANES), 0)

    def lookup(step, carry):
        base = pl.multiple_of(step * 8, 8)
        tile = ids_ref[pl.ds(base, 8), :]
        high, low = tile >> 7, tile & (LANES - 1)
        for k in range(0, 8, 2):
            hot = [(map_iota == high[q : q + 1, :]).astype(jnp.bfloat16) for q in (k, k + 1)]
            found = dot_tn(pieces, jnp.concatenate(hot, axis=1))
            found = found[:LANES] * 65536.0 + found[LANES : 2 * LANES] * 256.0 + found[2 * LANES :]
            lane = jnp.concatenate([low[k : k + 1, :], low[k + 1 : k + 2, :]], axis=1)
            picked = jnp.sum(jnp.where(lane_iota == lane, found, 0.0), axis=0, keepdims=True)
            pos_ref[pl.ds(base + k, 1), :] = picked[:, :LANES].astype(jnp.int32)
            pos_ref[pl.ds(base + k + 1, 1), :] = picked[:, LANES:].astype(jnp.int32)
        return carry

    lax.fori_loop(0, blocks, lookup, 0)
    position = pos_ref[...]
    owner = position >> shift
    local = position & ((1 << shift) - 1)
    row_iota = lax.broadcasted_iota(jnp.int32, (rows, LANES), 0)
    is_cold = (local >= HOT_DEV) & (row_iota < id_rows)
    owner_cold = jnp.where(is_cold, owner, -1)
    upper = (
        lax.broadcasted_iota(jnp.int32, (LANES, LANES), 0) <= lax.broadcasted_iota(jnp.int32, (LANES, LANES), 1)
    ).astype(jnp.bfloat16)
    ones = jnp.ones((LANES, LANES), jnp.bfloat16)
    below = (
        lax.broadcasted_iota(jnp.int32, (rows, rows), 1) < lax.broadcasted_iota(jnp.int32, (rows, rows), 0)
    ).astype(jnp.bfloat16)
    slot = jnp.full((rows, LANES), -1.0, jnp.float32)
    for part in range(parts):
        hit = owner_cold == part
        member = hit.astype(jnp.bfloat16)
        ahead = dot_nn(below, member).astype(jnp.bfloat16)
        running = dot_nn(member, upper) + dot_nn(ahead, ones)
        slot = jnp.where(hit, running - 1.0, slot)
    slot = slot.astype(jnp.int32)
    addr_ref[...] = owner * stride + jnp.where(is_cold, HOT_DEV + slot, local)
    own_ref[...] = owner_cold
    slot_ref[...] = slot
    val_ref[...] = local
    part_iota = lax.broadcasted_iota(jnp.int32, (parts, LANES), 0)
    slot_iota = lax.broadcasted_iota(jnp.int32, (cap_pad, LANES), 0)

    def place(step, table):
        base = pl.multiple_of(step * 8, 8)
        own8 = own_ref[pl.ds(base, 8), :]
        slot8 = slot_ref[pl.ds(base, 8), :]
        val8 = val_ref[pl.ds(base, 8), :]
        for k in range(0, 8, 2):
            lefts, rights = [], []
            for q in range(k, k + 2):
                val = val8[q : q + 1, :].astype(jnp.float32)
                top = jnp.floor(val * (1.0 / LANES))
                mine = part_iota == own8[q : q + 1, :]
                lefts.append(
                    jnp.concatenate(
                        [jnp.where(mine, top, 0.0), jnp.where(mine, val - top * LANES, 0.0)], axis=0
                    ).astype(jnp.bfloat16)
                )
                rights.append((slot_iota == slot8[q : q + 1, :]).astype(jnp.bfloat16))
            table = table + dot_nt(jnp.concatenate(lefts, axis=1), jnp.concatenate(rights, axis=1))
        return table

    table = lax.fori_loop(0, blocks, place, jnp.zeros((2 * parts, cap_pad), jnp.float32))
    request = (table[:parts] * LANES + table[parts:]).astype(jnp.int32)
    req_ref[...] = jnp.zeros(req_ref.shape, jnp.int32)
    for c in range(cap_pad // LANES):
        req_ref[:, c, :] = request[:, c * LANES : (c + 1) * LANES]


def plan(ids, partition_map, parts, node_rows, stride, id_rows, cap_pad):
    rows = ids.shape[0]
    kernel = functools.partial(
        plan_kernel,
        parts=parts,
        shift=node_rows.bit_length() - 1,
        stride=stride,
        id_rows=id_rows,
        cap_pad=cap_pad,
    )
    return pl.pallas_call(
        kernel,
        name="plan",
        out_shape=(
            jax.ShapeDtypeStruct((parts, round_up(cap_pad // LANES, 8), LANES), jnp.int32),
            jax.ShapeDtypeStruct((rows, LANES), jnp.int32),
        ),
        in_specs=[pl.BlockSpec(memory_space=pltpu.VMEM)] * 2,
        out_specs=(pl.BlockSpec(memory_space=pltpu.VMEM),) * 2,
        scratch_shapes=[pltpu.VMEM((rows, LANES), jnp.int32)] * 4,
        compiler_params=pltpu.CompilerParams(vmem_limit_bytes=VMEM_LIMIT),
        cost_estimate=pl.CostEstimate(flops=40_000_000, bytes_accessed=1_000_000, transcendentals=0),
    )(ids, partition_map.reshape(-1, LANES))


ROOT = 0.7978845608028654
CUBE = 0.044715


def gelu_pair(pre):
    square = pre * pre
    bend = jnp.tanh(ROOT * pre * (1.0 + CUBE * square))
    half = 0.5 * (1.0 + bend)
    slope = half + 0.5 * pre * (1.0 - bend * bend) * (ROOT * (1.0 + 3.0 * CUBE * square))
    return pre * half, slope


def tree_sum(values):
    while len(values) > 1:
        values = [a + b for a, b in zip(values[::2], values[1::2])] + (
            [values[-1]] if len(values) % 2 else []
        )
    return values[0]


def model_kernel(
    addr_ref, table_ref, label_ref, self_one, neigh_one, b_one_ref, self_two, neigh_two, b_two_ref,
    loss_ref, pack_ref,
    wide, x_buf, far_buf, own_buf, slope_buf, d_buf, *, seeds, fan_one, fan_two,
):
    feat = table_ref.shape[1]
    hidden = self_one.shape[1]
    hops = seeds * fan_one
    chunk = 64 if table_ref.shape[0] % 64 == 0 else 16

    def widen(step, carry):
        at = pl.ds(pl.multiple_of(step * chunk, chunk), chunk)
        wide[at, :] = table_ref[at, :].astype(jnp.float32)
        return carry

    lax.fori_loop(0, table_ref.shape[0] // chunk, widen, 0)

    def fetch(step, carry):
        j = step // (seeds // 8)
        block = step % (seeds // 8)
        base = pl.multiple_of(step * 8, 8)
        for k in range(8):
            hop = (block * 8 + k) * fan_one + j
            own_buf[pl.ds(base + k, 1), :] = wide[pl.ds(addr_ref[seeds + hop], 1), :]
            first = seeds + hops + hop * fan_two
            rows = [wide[pl.ds(addr_ref[first + m], 1), :] for m in range(fan_two)]
            far_buf[pl.ds(base + k, 1), :] = tree_sum(rows)
        return carry

    lax.fori_loop(0, hops // 8, fetch, 0)

    def fetch_seed(step, carry):
        base = pl.multiple_of(step * 8, 8)
        for k in range(8):
            own_buf[pl.ds(hops + base + k, 1), :] = wide[pl.ds(addr_ref[base + k], 1), :]
        return carry

    lax.fori_loop(0, seeds // 8, fetch_seed, 0)

    w_one = jnp.concatenate([self_one[...], neigh_one[...]], axis=0)
    w_two = jnp.concatenate([self_two[...], neigh_two[...]], axis=0)
    b_one = b_one_ref[...]
    row_sum = jnp.zeros((seeds, feat), jnp.float32)
    hid_sum = jnp.zeros((seeds, hidden), jnp.float32)
    for j in range(fan_one):
        at = slice(j * seeds, (j + 1) * seeds)
        own = own_buf[at, :]
        row_sum = row_sum + own
        x_buf[at, :feat] = own.astype(jnp.bfloat16)
        x_buf[at, feat:] = (far_buf[at, :] * (1.0 / fan_two)).astype(jnp.bfloat16)
    x_buf[hops:, :feat] = own_buf[hops:, :].astype(jnp.bfloat16)
    x_buf[hops:, feat:] = (row_sum * (1.0 / fan_one)).astype(jnp.bfloat16)
    act = None
    for j in range(fan_one + 1):
        at = slice(j * seeds, (j + 1) * seeds)
        act, slope = gelu_pair(dot_nn(x_buf[at, :], w_one) + b_one)
        act = act.astype(jnp.bfloat16)
        slope_buf[at, :] = slope
        if j < fan_one:
            hid_sum = hid_sum + act.astype(jnp.float32)
    hid = jnp.concatenate([act, (hid_sum * (1.0 / fan_one)).astype(jnp.bfloat16)], axis=1)
    logits = dot_nn(hid, w_two) + b_two_ref[...]
    shifted = logits - jnp.max(logits, axis=1, keepdims=True)
    log_probs = shifted - jnp.log(jnp.sum(jnp.exp(shifted), axis=1, keepdims=True))
    class_iota = lax.broadcasted_iota(jnp.int32, logits.shape, 1)
    diagonal = lax.broadcasted_iota(jnp.int32, (seeds, seeds), 0) == lax.broadcasted_iota(jnp.int32, (seeds, seeds), 1)
    label = jnp.sum(jnp.where(diagonal, label_ref[...].astype(jnp.float32), 0.0), axis=1, keepdims=True)
    target = (class_iota.astype(jnp.float32) == label).astype(jnp.float32)
    loss_ref[...] = -jnp.sum(log_probs * target, axis=1, keepdims=True)
    d_logits = ((jnp.exp(log_probs) - target) * (1.0 / seeds)).astype(jnp.bfloat16)
    g_two = dot_tn(hid, d_logits)
    gb_two = dot_tn(d_logits, jnp.ones((seeds, LANES), jnp.bfloat16))
    d_hid = dot_nt(d_logits, w_two)
    d_hop = d_hid[:, hidden:] * (1.0 / fan_one)
    for j in range(fan_one + 1):
        at = slice(j * seeds, (j + 1) * seeds)
        d_pre = ((d_hop if j < fan_one else d_hid[:, :hidden]) * slope_buf[at, :]).astype(jnp.bfloat16)
        d_buf[at, :] = d_pre
    gb_one = dot_tn(d_buf[...], jnp.ones((d_buf.shape[0], LANES), jnp.bfloat16))
    pack_gradients(pack_ref, dot_tn(x_buf[...], d_buf[...]), gb_one, g_two, gb_two)


def model(addr, table, labels, self_one, neigh_one, bias_one, self_two, neigh_two, bias_two, fan_one, fan_two, pack_rows):
    seeds = labels.shape[0]
    feat, hidden = self_one.shape
    classes = self_two.shape[1]
    total = seeds * (1 + fan_one)
    vmem = pl.BlockSpec(memory_space=pltpu.VMEM)
    return pl.pallas_call(
        functools.partial(model_kernel, seeds=seeds, fan_one=fan_one, fan_two=fan_two),
        name="model",
        out_shape=(
            jax.ShapeDtypeStruct((seeds, 1), jnp.float32),
            jax.ShapeDtypeStruct((pack_rows, LANES), jnp.float32),
        ),
        in_specs=[pl.BlockSpec(memory_space=pltpu.SMEM)] + [vmem] * 8,
        out_specs=(vmem,) * 2,
        scratch_shapes=[
            pltpu.VMEM(table.shape, jnp.float32),
            pltpu.VMEM((total, 2 * feat), jnp.bfloat16),
            pltpu.VMEM((total - seeds, feat), jnp.float32),
            pltpu.VMEM((total, feat), jnp.float32),
            pltpu.VMEM((total, hidden), jnp.float32),
            pltpu.VMEM((total, hidden), jnp.bfloat16),
        ],
        compiler_params=pltpu.CompilerParams(vmem_limit_bytes=VMEM_LIMIT),
        cost_estimate=pl.CostEstimate(flops=100_000_000, bytes_accessed=4_000_000, transcendentals=0),
    )(
        addr,
        table,
        labels.reshape(1, seeds),
        self_one,
        neigh_one,
        bias_one.reshape(1, hidden),
        self_two,
        neigh_two,
        bias_two.reshape(1, classes),
    )


def exchange_kernel(
    req_ref, feat_ref, out_ref, inbox, wanted, wide, stage, send,
    local_sem, req_send, req_recv, hub_send, hub_recv, row_send, row_recv, *, parts, asks,
):
    node_rows = feat_ref.shape[0]
    cap_row = send.shape[1]
    me = lax.axis_index("dom")
    bits = parts.bit_length() - 1
    barrier = pltpu.get_barrier_semaphore()

    def partner(mask):
        other = me ^ mask
        return other, {"dom": other}

    def greet(step, carry):
        pl.semaphore_signal(barrier, inc=1, device_id=partner(step)[1], device_id_type=MESH)
        return carry

    lax.fori_loop(1, parts, greet, 0)
    hub_at = pl.ds(0, HOT_DEV)
    ask_at = pl.ds(0, asks)
    keep_req = pltpu.make_async_copy(req_ref.at[me], inbox.at[me], local_sem.at[0])
    keep_req.start()
    keep_hub = pltpu.make_async_copy(feat_ref.at[hub_at], out_ref.at[me, hub_at], local_sem.at[1])
    keep_hub.start()
    pl.semaphore_wait(barrier, parts - 1)

    def ask(step, carry):
        other, at = partner(parts - step)
        pltpu.make_async_remote_copy(
            req_ref.at[other, ask_at], inbox.at[me, ask_at], req_send, req_recv, device_id=at, device_id_type=MESH
        ).start()
        return carry

    lax.fori_loop(1, parts, ask, 0)
    keep_hub.wait()

    def held(level, index):
        return me ^ (index * (parts >> level))

    def share(level):
        at = partner(parts >> (level + 1))[1]

        def one(index, carry):
            slot = held(level, index)
            pltpu.make_async_remote_copy(
                out_ref.at[slot, hub_at], out_ref.at[slot, hub_at], hub_send.at[level], hub_recv.at[level],
                device_id=at, device_id_type=MESH,
            ).start()
            return carry

        lax.fori_loop(0, 1 << level, one, 0)

    def shared(level):
        some = out_ref.at[pl.ds(0, 1 << level), hub_at]
        return pltpu.make_async_remote_copy(
            some, some, hub_send.at[level], hub_recv.at[level], device_id=partner(1)[1], device_id_type=MESH
        )

    share(0)

    def widen(step, carry):
        at = pl.ds(pl.multiple_of(step * 64, 64), 64)
        wide[at, :] = feat_ref[at, :].astype(jnp.float32)
        return carry

    lax.fori_loop(0, node_rows // 64, widen, 0)
    most = pl.ds(0, parts - 1)
    asked = pltpu.make_async_remote_copy(
        req_ref.at[most, ask_at], inbox.at[most, ask_at], req_send, req_recv,
        device_id=partner(1)[1], device_id_type=MESH,
    )
    keep_req.wait()
    asked.wait_recv()
    to_scalar = pltpu.make_async_copy(inbox.at[:, ask_at], wanted, local_sem.at[2])
    to_scalar.start()
    to_scalar.wait()

    def collect(other):
        def block(step, carry):
            base = pl.multiple_of(step * 16, 16)
            row = step // (LANES // 16)
            lane = lax.rem(step, LANES // 16) * 16
            for k in range(16):
                stage[pl.ds(base + k, 1), :] = wide[pl.ds(wanted[other, row, lane + k], 1), :]
            return carry

        lax.fori_loop(0, cap_row // 16, block, 0)
        return stage[...].astype(jnp.bfloat16)

    rows_at = pl.ds(HOT_DEV, cap_row)

    def serve(step, carry):
        other, at = partner(parts - step)
        send[other] = collect(other)
        pltpu.make_async_remote_copy(
            send.at[other], out_ref.at[me, rows_at], row_send, row_recv, device_id=at, device_id_type=MESH
        ).start()
        return carry

    served = 1
    for level in range(1, bits):
        until = parts * level // bits
        lax.fori_loop(served, until, serve, 0)
        served = until
        shared(level - 1).wait_recv()
        share(level)
    lax.fori_loop(served, parts, serve, 0)
    out_ref[me, HOT_DEV:, :] = collect(me)
    rows = pltpu.make_async_remote_copy(
        send.at[most], out_ref.at[most, rows_at], row_send, row_recv, device_id=partner(1)[1], device_id_type=MESH
    )
    asked.wait_send()
    shared(bits - 1).wait_recv()
    for level in range(bits):
        shared(level).wait_send()
    rows.wait()


def exchange(request, features, cap_row, asks):
    parts = lax.axis_size("dom")
    bits = parts.bit_length() - 1
    node_rows, feat = features.shape
    vmem = pl.BlockSpec(memory_space=pltpu.VMEM)
    return pl.pallas_call(
        functools.partial(exchange_kernel, parts=parts, asks=asks),
        name="exchange",
        out_shape=jax.ShapeDtypeStruct((parts, HOT_DEV + cap_row, feat), features.dtype),
        in_specs=[vmem, vmem],
        out_specs=vmem,
        scratch_shapes=[
            pltpu.VMEM(request.shape, jnp.int32),
            pltpu.SMEM((parts, asks, LANES), jnp.int32),
            pltpu.VMEM((node_rows, feat), jnp.float32),
            pltpu.VMEM((cap_row, feat), jnp.float32),
            pltpu.VMEM((parts, cap_row, feat), features.dtype),
            pltpu.SemaphoreType.DMA((3,)),
            pltpu.SemaphoreType.DMA,
            pltpu.SemaphoreType.DMA,
            pltpu.SemaphoreType.DMA((bits,)),
            pltpu.SemaphoreType.DMA((bits,)),
            pltpu.SemaphoreType.DMA,
            pltpu.SemaphoreType.DMA,
        ],
        compiler_params=pltpu.CompilerParams(collective_id=2, has_side_effects=True, vmem_limit_bytes=VMEM_LIMIT),
    )(request, features)


def pack_plan(feat, hidden):
    halves = hidden // LANES
    one = 2 * feat * halves
    low = one + 2 * hidden
    return halves, one, low, low + hidden


def pack_gradients(pack_ref, g_one, gb_one, g_two, gb_two):
    hidden, feat = g_one.shape[1], g_one.shape[0] // 2
    classes = g_two.shape[1]
    halves, one, low, used = pack_plan(feat, hidden)
    for h in range(halves):
        pack_ref[h * 2 * feat : (h + 1) * 2 * feat, :] = g_one[:, h * LANES : (h + 1) * LANES]
    pack_ref[one:low, :] = g_two[:, :LANES]
    rest = classes - LANES
    space = LANES // 2 - rest
    second = jnp.concatenate([gb_two[:, :1], jnp.zeros((hidden - classes, 1), jnp.float32)], axis=0)
    pack_ref[low:used, :] = jnp.concatenate(
        [
            g_two[:hidden, LANES:], gb_one[:, :1], second, jnp.zeros((hidden, space - 2), jnp.float32),
            g_two[hidden:, LANES:], jnp.zeros((hidden, space), jnp.float32),
        ],
        axis=1,
    )
    if pack_ref.shape[0] > used:
        pack_ref[used:, :] = jnp.zeros((pack_ref.shape[0] - used, LANES), jnp.float32)


def unpack_kernel(pack_ref, self_one, neigh_one, bias_one, self_two, neigh_two, bias_two):
    feat, hidden = self_one.shape
    classes = self_two.shape[1]
    rest = classes - LANES
    halves, one, low, used = pack_plan(feat, hidden)
    for h in range(halves):
        cols = slice(h * LANES, (h + 1) * LANES)
        at = h * 2 * feat
        self_one[:, cols] = pack_ref[at : at + feat, :]
        neigh_one[:, cols] = pack_ref[at + feat : at + 2 * feat, :]
    self_two[:, :LANES] = pack_ref[one : one + hidden, :]
    neigh_two[:, :LANES] = pack_ref[one + hidden : low, :]
    high = pack_ref[low:used, :]
    self_two[:, LANES:] = high[:, :rest]
    neigh_two[:, LANES:] = high[:, LANES // 2 : LANES // 2 + rest]
    turned = high.T
    bias_one[...] = turned[rest : rest + 1, :]
    bias_two[...] = turned[rest + 1 : rest + 2, :classes]


def unpack(packed, feat, hidden, classes):
    vmem = pl.BlockSpec(memory_space=pltpu.VMEM)
    shapes = [(feat, hidden), (feat, hidden), (1, hidden), (hidden, classes), (hidden, classes), (1, classes)]
    return pl.pallas_call(
        unpack_kernel,
        name="unpack",
        out_shape=tuple(jax.ShapeDtypeStruct(shape, jnp.float32) for shape in shapes),
        in_specs=[vmem],
        out_specs=(vmem,) * 6,
        compiler_params=pltpu.CompilerParams(vmem_limit_bytes=VMEM_LIMIT),
    )(packed)


def reduce_kernel(
    part_ref, out_ref, near_box, middle, far_box, gathered, send_sem, recv_sem, *, n_dom, n_rep, near,
):
    count = n_dom * n_rep
    far = count // near
    rows = part_ref.shape[0] // count
    span = far * rows
    me = lax.axis_index("dom") * n_rep + lax.axis_index("rep")
    here, there = lax.rem(me, near), me // near
    barrier = pltpu.get_barrier_semaphore()

    def place(index):
        return {"dom": index // n_rep, "rep": lax.rem(index, n_rep)}

    def near_peer(step):
        other = lax.rem(here + step, near)
        return other, place(there * near + other)

    def far_peer(step):
        other = lax.rem(there + step, far)
        return other, place(other * near + here)

    def wide_at(index):
        return pl.ds(pl.multiple_of(index * span, 8), span)

    def thin_at(index):
        return pl.ds(pl.multiple_of(index * rows, 8), rows)

    def greet_near(step, carry):
        pl.semaphore_signal(barrier, inc=1, device_id=near_peer(step)[1], device_id_type=MESH)
        return carry

    def greet_far(step, carry):
        pl.semaphore_signal(barrier, inc=1, device_id=far_peer(step)[1], device_id_type=MESH)
        return carry

    lax.fori_loop(1, near, greet_near, 0)
    lax.fori_loop(1, far, greet_far, 0)
    pl.semaphore_wait(barrier, near + far - 2)

    def copy(source, target, stage, where):
        return pltpu.make_async_remote_copy(
            source, target, send_sem.at[stage], recv_sem.at[stage], device_id=where, device_id_type=MESH
        )

    def out_near(step, carry):
        other, where = near_peer(step)
        copy(part_ref.at[wide_at(other)], near_box.at[wide_at(here)], 0, where).start()
        return carry

    lax.fori_loop(1, near, out_near, 0)
    some = pl.ds(0, (near - 1) * span)
    first = copy(part_ref.at[some], near_box.at[some], 0, near_peer(1)[1])
    first.wait_recv()

    def add_near(step, total):
        return total + near_box[wide_at(near_peer(step)[0]), :]

    middle[...] = lax.fori_loop(1, near, add_near, part_ref[wide_at(here), :])

    def out_far(step, carry):
        other, where = far_peer(step)
        copy(middle.at[thin_at(other)], far_box.at[thin_at(there)], 1, where).start()
        return carry

    lax.fori_loop(1, far, out_far, 0)
    some = pl.ds(0, (far - 1) * rows)
    second = copy(middle.at[some], far_box.at[some], 1, far_peer(1)[1])
    second.wait_recv()

    def add_far(step, total):
        return total + far_box[thin_at(far_peer(step)[0]), :]

    total = lax.fori_loop(1, far, add_far, middle[thin_at(there), :])
    mine = here * far + there
    gathered[mine] = total.astype(gathered.dtype)

    def back_far(step, carry):
        copy(gathered.at[mine], gathered.at[mine], 2, far_peer(step)[1]).start()
        return carry

    lax.fori_loop(1, far, back_far, 0)
    some = gathered.at[pl.ds(0, far - 1)]
    third = copy(some, some, 2, far_peer(1)[1])
    third.wait_recv()
    group = gathered.at[pl.ds(here * far, far)]

    def back_near(step, carry):
        copy(group, group, 3, near_peer(step)[1]).start()
        return carry

    lax.fori_loop(1, near, back_near, 0)
    some = gathered.at[pl.ds(0, (near - 1) * far)]
    fourth = copy(some, some, 3, near_peer(1)[1])
    fourth.wait_recv()
    first.wait_send()
    second.wait_send()
    third.wait_send()
    fourth.wait_send()
    for index in range(count):
        out_ref[index * rows : (index + 1) * rows, :] = gathered[index].astype(jnp.float32)


def sum_everywhere(pieces):
    n_dom, n_rep = lax.axis_size("dom"), lax.axis_size("rep")
    count = n_dom * n_rep
    near = 8
    far = count // near
    rows = pieces.shape[0] // count
    vmem = pl.BlockSpec(memory_space=pltpu.VMEM)
    return pl.pallas_call(
        functools.partial(reduce_kernel, n_dom=n_dom, n_rep=n_rep, near=near),
        name="sum_everywhere",
        out_shape=jax.ShapeDtypeStruct(pieces.shape, jnp.float32),
        in_specs=[vmem],
        out_specs=vmem,
        scratch_shapes=[
            pltpu.VMEM(pieces.shape, jnp.float32),
            pltpu.VMEM((far * rows, LANES), jnp.float32),
            pltpu.VMEM((far * rows, LANES), jnp.float32),
            pltpu.VMEM((count, rows, LANES), jnp.bfloat16),
            pltpu.SemaphoreType.DMA((4,)),
            pltpu.SemaphoreType.DMA((4,)),
        ],
        compiler_params=pltpu.CompilerParams(collective_id=1, has_side_effects=True, vmem_limit_bytes=VMEM_LIMIT),
    )(pieces)


def shards(
    features, partition_map, seed_ids, hop1_ids, hop2_ids, labels,
    self_one, neigh_one, bias_one, self_two, neigh_two, bias_two,
):
    parts = lax.axis_size("dom")
    count = parts * lax.axis_size("rep")
    seeds = seed_ids.shape[0]
    fan_one = hop1_ids.shape[1]
    fan_two = hop2_ids.shape[2]
    node_rows, feat = features.shape
    tree_rows = 1 + fan_one + fan_one * fan_two
    cold_cap = tree_rows // 2 * (seeds // parts)
    cap_row = round_up(cold_cap, 16)
    cap_pad = round_up(cold_cap, LANES)
    stride = HOT_DEV + cap_row
    total = seeds * tree_rows
    id_rows = total // LANES
    wanted = jnp.concatenate([seed_ids, hop1_ids.reshape(-1), hop2_ids.reshape(-1)])
    ids = jnp.pad(wanted.reshape(id_rows, LANES), ((0, round_up(id_rows, 8) - id_rows), (0, 0)))
    request, addr = plan(ids, partition_map, parts, node_rows, stride, id_rows, cap_pad)
    table = exchange(request, features, cap_row, cap_pad // LANES).reshape(parts * stride, feat)
    hidden, classes = self_two.shape
    used = pack_plan(feat, hidden)[-1]
    pack_rows = count * round_up(-(-used // count), 8)
    loss, pieces = model(
        addr.reshape(-1), table, labels, self_one, neigh_one, bias_one, self_two, neigh_two, bias_two,
        fan_one, fan_two, pack_rows,
    )
    grads = unpack(sum_everywhere(pieces), feat, hidden, classes)
    return (
        loss.reshape(-1), grads[0], grads[1], grads[2].reshape(-1),
        grads[3], grads[4], grads[5].reshape(-1),
    )


def solution(mesh):
    return jax.shard_map(
        shards,
        mesh=mesh,
        in_specs=(
            P("dom", None),
            P(),
            P(("dom", "rep")),
            P(("dom", "rep"), None),
            P(("dom", "rep"), None, None),
            P(("dom", "rep")),
            P(),
            P(),
            P(),
            P(),
            P(),
            P(),
        ),
        out_specs=(P(("dom", "rep")), P(), P(), P(), P(), P(), P()),
        check_vma=False,
    )
```

```python
import functools

import jax
import jax.numpy as jnp
from jax import lax
from jax.experimental import pallas as pl
from jax.experimental.pallas import tpu as pltpu
from jax.sharding import PartitionSpec as P

HOT_DEV = 256
LANES = 128
MESH = pl.DeviceIdType.MESH
VMEM_LIMIT = 56 * 1024 * 1024


def round_up(value, unit):
    return -(-value // unit) * unit


def dot_tn(left, right):
    return lax.dot_general(left, right, (((0,), (0,)), ((), ())), preferred_element_type=jnp.float32)


def dot_nt(left, right):
    return lax.dot_general(left, right, (((1,), (1,)), ((), ())), preferred_element_type=jnp.float32)


def dot_nn(left, right):
    return jnp.dot(left, right, preferred_element_type=jnp.float32)


def plan_kernel(ids_ref, map_ref, req_ref, addr_ref, own_ref, slot_ref, val_ref, pos_ref, pieces_ref, *, parts, shift, stride, id_rows, cap_pad):
    rows = ids_ref.shape[0]
    blocks = rows // 8
    stored = map_ref[...]
    pieces = jnp.concatenate([stored >> 16, (stored >> 8) & 255, stored & 255], axis=1)
    pieces_ref[...] = pieces.astype(jnp.float32).T.astype(jnp.bfloat16)
    map_iota = lax.broadcasted_iota(jnp.int32, map_ref.shape, 0)
    lane_iota = lax.broadcasted_iota(jnp.int32, (LANES, 2 * LANES), 0)

    def lookup(step, carry):
        base = pl.multiple_of(step * 8, 8)
        tile = ids_ref[pl.ds(base, 8), :]
        high, low = tile >> 7, tile & (LANES - 1)
        for k in range(0, 8, 2):
            hot = [(map_iota == high[q : q + 1, :]).astype(jnp.bfloat16) for q in (k, k + 1)]
            found = dot_nn(pieces_ref[...], jnp.concatenate(hot, axis=1))
            found = found[:LANES] * 65536.0 + found[LANES : 2 * LANES] * 256.0 + found[2 * LANES :]
            lane = jnp.concatenate([low[k : k + 1, :], low[k + 1 : k + 2, :]], axis=1)
            picked = jnp.sum(jnp.where(lane_iota == lane, found, 0.0), axis=0, keepdims=True)
            pos_ref[pl.ds(base + k, 1), :] = picked[:, :LANES].astype(jnp.int32)
            pos_ref[pl.ds(base + k + 1, 1), :] = picked[:, LANES:].astype(jnp.int32)
        return carry

    lax.fori_loop(0, blocks, lookup, 0)
    position = pos_ref[...]
    owner = position >> shift
    local = position & ((1 << shift) - 1)
    row_iota = lax.broadcasted_iota(jnp.int32, (rows, LANES), 0)
    is_cold = (local >= HOT_DEV) & (row_iota < id_rows)
    owner_cold = jnp.where(is_cold, owner, -1)
    upper = (
        lax.broadcasted_iota(jnp.int32, (LANES, LANES), 0) <= lax.broadcasted_iota(jnp.int32, (LANES, LANES), 1)
    ).astype(jnp.bfloat16)
    ones = jnp.ones((LANES, LANES), jnp.bfloat16)
    below = (
        lax.broadcasted_iota(jnp.int32, (rows, rows), 1) < lax.broadcasted_iota(jnp.int32, (rows, rows), 0)
    ).astype(jnp.bfloat16)
    slot = jnp.full((rows, LANES), -1.0, jnp.float32)
    for part in range(parts):
        hit = owner_cold == part
        member = hit.astype(jnp.bfloat16)
        ahead = dot_nn(below, member).astype(jnp.bfloat16)
        running = dot_nn(member, upper) + dot_nn(ahead, ones)
        slot = jnp.where(hit, running - 1.0, slot)
    slot = slot.astype(jnp.int32)
    addr_ref[...] = owner * stride + jnp.where(is_cold, HOT_DEV + slot, local)
    own_ref[...] = owner_cold
    slot_ref[...] = slot
    val_ref[...] = local
    part_iota = lax.broadcasted_iota(jnp.int32, (parts, LANES), 0)
    slot_iota = lax.broadcasted_iota(jnp.int32, (cap_pad, LANES), 0)

    def place(step, table):
        base = pl.multiple_of(step * 8, 8)
        own8 = own_ref[pl.ds(base, 8), :]
        slot8 = slot_ref[pl.ds(base, 8), :]
        val8 = val_ref[pl.ds(base, 8), :]
        for k in range(0, 8, 2):
            lefts, rights = [], []
            for q in range(k, k + 2):
                val = val8[q : q + 1, :].astype(jnp.float32)
                top = jnp.floor(val * (1.0 / LANES))
                mine = part_iota == own8[q : q + 1, :]
                lefts.append(
                    jnp.concatenate(
                        [jnp.where(mine, top, 0.0), jnp.where(mine, val - top * LANES, 0.0)], axis=0
                    ).astype(jnp.bfloat16)
                )
                rights.append((slot_iota == slot8[q : q + 1, :]).astype(jnp.bfloat16))
            table = table + dot_nt(jnp.concatenate(lefts, axis=1), jnp.concatenate(rights, axis=1))
        return table

    table = lax.fori_loop(0, blocks, place, jnp.zeros((2 * parts, cap_pad), jnp.float32))
    request = (table[:parts] * LANES + table[parts:]).astype(jnp.int32)
    req_ref[...] = jnp.zeros(req_ref.shape, jnp.int32)
    for c in range(cap_pad // LANES):
        req_ref[:, c, :] = request[:, c * LANES : (c + 1) * LANES]


def plan(ids, partition_map, parts, node_rows, stride, id_rows, cap_pad):
    rows = ids.shape[0]
    kernel = functools.partial(
        plan_kernel,
        parts=parts,
        shift=node_rows.bit_length() - 1,
        stride=stride,
        id_rows=id_rows,
        cap_pad=cap_pad,
    )
    return pl.pallas_call(
        kernel,
        name="plan",
        out_shape=(
            jax.ShapeDtypeStruct((parts, round_up(cap_pad // LANES, 8), LANES), jnp.int32),
            jax.ShapeDtypeStruct((rows, LANES), jnp.int32),
        ),
        in_specs=[pl.BlockSpec(memory_space=pltpu.VMEM)] * 2,
        out_specs=(pl.BlockSpec(memory_space=pltpu.VMEM),) * 2,
        scratch_shapes=[pltpu.VMEM((rows, LANES), jnp.int32)] * 4
        + [pltpu.VMEM((3 * LANES, partition_map.size // LANES), jnp.bfloat16)],
        compiler_params=pltpu.CompilerParams(vmem_limit_bytes=VMEM_LIMIT),
        cost_estimate=pl.CostEstimate(flops=40_000_000, bytes_accessed=1_000_000, transcendentals=0),
    )(ids, partition_map.reshape(-1, LANES))


ROOT = 0.7978845608028654
CUBE = 0.044715


def gelu_pair(pre):
    square = pre * pre
    bend = jnp.tanh(ROOT * pre * (1.0 + CUBE * square))
    half = 0.5 * (1.0 + bend)
    slope = half + 0.5 * pre * (1.0 - bend * bend) * (ROOT * (1.0 + 3.0 * CUBE * square))
    return pre * half, slope


def tree_sum(values):
    while len(values) > 1:
        values = [a + b for a, b in zip(values[::2], values[1::2])] + (
            [values[-1]] if len(values) % 2 else []
        )
    return values[0]


def model_kernel(
    addr_ref, table_ref, label_ref, self_one, neigh_one, b_one_ref, self_two, neigh_two, b_two_ref,
    loss_ref, pack_ref,
    wide, x_buf, far_buf, own_buf, slope_buf, d_buf, *, seeds, fan_one, fan_two,
):
    feat = table_ref.shape[1]
    hidden = self_one.shape[1]
    hops = seeds * fan_one
    chunk = 64 if table_ref.shape[0] % 64 == 0 else 16

    def widen(step, carry):
        at = pl.ds(pl.multiple_of(step * chunk, chunk), chunk)
        wide[at, :] = table_ref[at, :].astype(jnp.float32)
        return carry

    lax.fori_loop(0, table_ref.shape[0] // chunk, widen, 0)

    def fetch(step, carry):
        j = step // (seeds // 8)
        block = step % (seeds // 8)
        base = pl.multiple_of(step * 8, 8)
        for k in range(8):
            hop = (block * 8 + k) * fan_one + j
            own_buf[pl.ds(base + k, 1), :] = wide[pl.ds(addr_ref[seeds + hop], 1), :]
            first = seeds + hops + hop * fan_two
            rows = [wide[pl.ds(addr_ref[first + m], 1), :] for m in range(fan_two)]
            far_buf[pl.ds(base + k, 1), :] = tree_sum(rows)
        return carry

    lax.fori_loop(0, hops // 8, fetch, 0)

    def fetch_seed(step, carry):
        base = pl.multiple_of(step * 8, 8)
        for k in range(8):
            own_buf[pl.ds(hops + base + k, 1), :] = wide[pl.ds(addr_ref[base + k], 1), :]
        return carry

    lax.fori_loop(0, seeds // 8, fetch_seed, 0)

    w_one = jnp.concatenate([self_one[...], neigh_one[...]], axis=0)
    w_two = jnp.concatenate([self_two[...], neigh_two[...]], axis=1)
    b_one = b_one_ref[...]
    row_sum = jnp.zeros((seeds, feat), jnp.float32)
    hid_sum = jnp.zeros((seeds, hidden), jnp.float32)
    for j in range(fan_one):
        at = slice(j * seeds, (j + 1) * seeds)
        own = own_buf[at, :]
        row_sum = row_sum + own
        x_buf[at, :feat] = own.astype(jnp.bfloat16)
        x_buf[at, feat:] = (far_buf[at, :] * (1.0 / fan_two)).astype(jnp.bfloat16)
    x_buf[hops:, :feat] = own_buf[hops:, :].astype(jnp.bfloat16)
    x_buf[hops:, feat:] = (row_sum * (1.0 / fan_one)).astype(jnp.bfloat16)
    act = None
    for j in range(fan_one + 1):
        at = slice(j * seeds, (j + 1) * seeds)
        act, slope = gelu_pair(dot_nn(x_buf[at, :], w_one) + b_one)
        act = act.astype(jnp.bfloat16)
        slope_buf[at, :] = slope
        if j < fan_one:
            hid_sum = hid_sum + act.astype(jnp.float32)
    hid = jnp.concatenate([act, (hid_sum * (1.0 / fan_one)).astype(jnp.bfloat16)], axis=1)
    logits = dot_nt(hid, w_two) + b_two_ref[...]
    shifted = logits - jnp.max(logits, axis=1, keepdims=True)
    log_probs = shifted - jnp.log(jnp.sum(jnp.exp(shifted), axis=1, keepdims=True))
    class_iota = lax.broadcasted_iota(jnp.int32, logits.shape, 1)
    diagonal = lax.broadcasted_iota(jnp.int32, (seeds, seeds), 0) == lax.broadcasted_iota(jnp.int32, (seeds, seeds), 1)
    label = jnp.sum(jnp.where(diagonal, label_ref[...].astype(jnp.float32), 0.0), axis=1, keepdims=True)
    target = (class_iota.astype(jnp.float32) == label).astype(jnp.float32)
    loss = jnp.sum(log_probs * target, axis=1, keepdims=True)
    loss_ref[...] = -jnp.sum(jnp.where(diagonal, loss, 0.0), axis=0, keepdims=True)
    d_logits = ((jnp.exp(log_probs) - target) * (1.0 / seeds)).astype(jnp.bfloat16)
    g_two = dot_tn(d_logits, hid)
    gb_two = jnp.sum(d_logits.astype(jnp.float32), axis=0, keepdims=True)
    d_hid = dot_nn(d_logits, w_two)
    d_hop = d_hid[:, hidden:] * (1.0 / fan_one)
    for j in range(fan_one + 1):
        at = slice(j * seeds, (j + 1) * seeds)
        d_pre = ((d_hop if j < fan_one else d_hid[:, :hidden]) * slope_buf[at, :]).astype(jnp.bfloat16)
        d_buf[at, :] = d_pre
    gb_one = dot_nn(jnp.ones((8, d_buf.shape[0]), jnp.bfloat16), d_buf[...])[:1]
    pack_gradients(pack_ref, dot_tn(x_buf[...], d_buf[...]), gb_one, g_two, gb_two)


def model(addr, table, labels, self_one, neigh_one, bias_one, self_two, neigh_two, bias_two, fan_one, fan_two, pack_rows):
    seeds = labels.shape[0]
    feat, hidden = self_one.shape
    classes = self_two.shape[1]
    total = seeds * (1 + fan_one)
    vmem = pl.BlockSpec(memory_space=pltpu.VMEM)
    return pl.pallas_call(
        functools.partial(model_kernel, seeds=seeds, fan_one=fan_one, fan_two=fan_two),
        name="model",
        out_shape=(
            jax.ShapeDtypeStruct((1, seeds), jnp.float32),
            jax.ShapeDtypeStruct((pack_rows, LANES), jnp.float32),
        ),
        in_specs=[pl.BlockSpec(memory_space=pltpu.SMEM)] + [vmem] * 8,
        out_specs=(vmem,) * 2,
        scratch_shapes=[
            pltpu.VMEM(table.shape, jnp.float32),
            pltpu.VMEM((total, 2 * feat), jnp.bfloat16),
            pltpu.VMEM((total - seeds, feat), jnp.float32),
            pltpu.VMEM((total, feat), jnp.float32),
            pltpu.VMEM((total, hidden), jnp.float32),
            pltpu.VMEM((total, hidden), jnp.bfloat16),
        ],
        compiler_params=pltpu.CompilerParams(vmem_limit_bytes=VMEM_LIMIT),
        cost_estimate=pl.CostEstimate(flops=100_000_000, bytes_accessed=4_000_000, transcendentals=0),
    )(
        addr,
        table,
        labels.reshape(1, seeds),
        self_one,
        neigh_one,
        bias_one.reshape(1, hidden),
        self_two.T,
        neigh_two.T,
        bias_two.reshape(1, classes),
    )


def exchange_kernel(
    req_ref, feat_ref, out_ref, inbox, wanted, wide, stage, send,
    local_sem, req_send, req_recv, hub_send, hub_recv, row_send, row_recv, *, parts, asks,
):
    node_rows = feat_ref.shape[0]
    cap_row = send.shape[1]
    me = lax.axis_index("dom")
    bits = parts.bit_length() - 1
    barrier = pltpu.get_barrier_semaphore()

    def partner(mask):
        other = me ^ mask
        return other, {"dom": other}

    def greet(step, carry):
        pl.semaphore_signal(barrier, inc=1, device_id=partner(step)[1], device_id_type=MESH)
        return carry

    lax.fori_loop(1, parts, greet, 0)
    hub_at = pl.ds(0, HOT_DEV)
    ask_at = pl.ds(0, asks)
    keep_req = pltpu.make_async_copy(req_ref.at[me], inbox.at[me], local_sem.at[0])
    keep_req.start()
    keep_hub = pltpu.make_async_copy(feat_ref.at[hub_at], out_ref.at[me, hub_at], local_sem.at[1])
    keep_hub.start()
    pl.semaphore_wait(barrier, parts - 1)

    def ask(step, carry):
        other, at = partner(parts - step)
        pltpu.make_async_remote_copy(
            req_ref.at[other, ask_at], inbox.at[me, ask_at], req_send, req_recv, device_id=at, device_id_type=MESH
        ).start()
        return carry

    lax.fori_loop(1, parts, ask, 0)
    keep_hub.wait()

    def held(level, index):
        return me ^ (index * (parts >> level))

    def share(level):
        at = partner(parts >> (level + 1))[1]

        def one(index, carry):
            slot = held(level, index)
            pltpu.make_async_remote_copy(
                out_ref.at[slot, hub_at], out_ref.at[slot, hub_at], hub_send.at[level], hub_recv.at[level],
                device_id=at, device_id_type=MESH,
            ).start()
            return carry

        lax.fori_loop(0, 1 << level, one, 0)

    def shared(level):
        some = out_ref.at[pl.ds(0, 1 << level), hub_at]
        return pltpu.make_async_remote_copy(
            some, some, hub_send.at[level], hub_recv.at[level], device_id=partner(1)[1], device_id_type=MESH
        )

    share(0)

    def widen(step, carry):
        at = pl.ds(pl.multiple_of(step * 64, 64), 64)
        wide[at, :] = feat_ref[at, :].astype(jnp.float32)
        return carry

    lax.fori_loop(0, node_rows // 64, widen, 0)
    most = pl.ds(0, parts - 1)
    asked = pltpu.make_async_remote_copy(
        req_ref.at[most, ask_at], inbox.at[most, ask_at], req_send, req_recv,
        device_id=partner(1)[1], device_id_type=MESH,
    )
    keep_req.wait()
    asked.wait_recv()
    to_scalar = pltpu.make_async_copy(inbox.at[:, ask_at], wanted, local_sem.at[2])
    to_scalar.start()
    to_scalar.wait()

    def collect(other):
        def block(step, carry):
            base = pl.multiple_of(step * 16, 16)
            row = step // (LANES // 16)
            lane = lax.rem(step, LANES // 16) * 16
            for k in range(16):
                stage[pl.ds(base + k, 1), :] = wide[pl.ds(wanted[other, row, lane + k], 1), :]
            return carry

        lax.fori_loop(0, cap_row // 16, block, 0)
        return stage[...].astype(jnp.bfloat16)

    rows_at = pl.ds(HOT_DEV, cap_row)

    def serve(step, carry):
        other, at = partner(parts - step)
        send[other] = collect(other)
        pltpu.make_async_remote_copy(
            send.at[other], out_ref.at[me, rows_at], row_send, row_recv, device_id=at, device_id_type=MESH
        ).start()
        return carry

    served = 1
    for level in range(1, bits):
        until = parts * level // bits
        lax.fori_loop(served, until, serve, 0)
        served = until
        shared(level - 1).wait_recv()
        share(level)
    lax.fori_loop(served, parts, serve, 0)
    out_ref[me, HOT_DEV:, :] = collect(me)
    rows = pltpu.make_async_remote_copy(
        send.at[most], out_ref.at[most, rows_at], row_send, row_recv, device_id=partner(1)[1], device_id_type=MESH
    )
    asked.wait_send()
    shared(bits - 1).wait_recv()
    for level in range(bits):
        shared(level).wait_send()
    rows.wait()


def exchange(request, features, cap_row, asks):
    parts = lax.axis_size("dom")
    bits = parts.bit_length() - 1
    node_rows, feat = features.shape
    vmem = pl.BlockSpec(memory_space=pltpu.VMEM)
    return pl.pallas_call(
        functools.partial(exchange_kernel, parts=parts, asks=asks),
        name="exchange",
        out_shape=jax.ShapeDtypeStruct((parts, HOT_DEV + cap_row, feat), features.dtype),
        in_specs=[vmem, vmem],
        out_specs=vmem,
        scratch_shapes=[
            pltpu.VMEM(request.shape, jnp.int32),
            pltpu.SMEM((parts, asks, LANES), jnp.int32),
            pltpu.VMEM((node_rows, feat), jnp.float32),
            pltpu.VMEM((cap_row, feat), jnp.float32),
            pltpu.VMEM((parts, cap_row, feat), features.dtype),
            pltpu.SemaphoreType.DMA((3,)),
            pltpu.SemaphoreType.DMA,
            pltpu.SemaphoreType.DMA,
            pltpu.SemaphoreType.DMA((bits,)),
            pltpu.SemaphoreType.DMA((bits,)),
            pltpu.SemaphoreType.DMA,
            pltpu.SemaphoreType.DMA,
        ],
        compiler_params=pltpu.CompilerParams(collective_id=2, has_side_effects=True, vmem_limit_bytes=VMEM_LIMIT),
    )(request, features)


def pack_plan(feat, hidden, classes):
    halves = hidden // LANES
    one = 2 * feat * halves
    high = round_up(classes, 8)
    tail = one + 2 * halves * high
    return halves, one, high, tail, tail + 8


def pack_gradients(pack_ref, g_one, gb_one, g_two, gb_two):
    hidden, feat = g_one.shape[1], g_one.shape[0] // 2
    classes = g_two.shape[0]
    halves, one, high, tail, used = pack_plan(feat, hidden, classes)
    for h in range(halves):
        pack_ref[h * 2 * feat : (h + 1) * 2 * feat, :] = g_one[:, h * LANES : (h + 1) * LANES]
    pack_ref[one:, :] = jnp.zeros((pack_ref.shape[0] - one, LANES), jnp.float32)
    for h in range(2 * halves):
        pack_ref[one + h * high : one + h * high + classes, :] = g_two[:, h * LANES : (h + 1) * LANES]
    for h in range(halves):
        pack_ref[tail + h : tail + h + 1, :] = gb_one[:, h * LANES : (h + 1) * LANES]
    pack_ref[tail + halves : tail + halves + 1, :] = gb_two[:, :LANES]
    pack_ref[tail + halves + 1 : tail + halves + 2, : classes - LANES] = gb_two[:, LANES:]


def unpack_kernel(pack_ref, self_one, neigh_one, bias_one, self_two, neigh_two, bias_two):
    feat, hidden = self_one.shape
    classes = self_two.shape[0]
    halves, one, high, tail, used = pack_plan(feat, hidden, classes)
    for h in range(halves):
        cols = slice(h * LANES, (h + 1) * LANES)
        at = h * 2 * feat
        self_one[:, cols] = pack_ref[at : at + feat, :]
        neigh_one[:, cols] = pack_ref[at + feat : at + 2 * feat, :]
        at = one + h * high
        self_two[:, cols] = pack_ref[at : at + classes, :]
        at = one + (halves + h) * high
        neigh_two[:, cols] = pack_ref[at : at + classes, :]
        bias_one[:, cols] = pack_ref[tail + h : tail + h + 1, :]
    bias_two[:, :LANES] = pack_ref[tail + halves : tail + halves + 1, :]
    bias_two[:, LANES:] = pack_ref[tail + halves + 1 : tail + halves + 2, : classes - LANES]


def unpack(packed, feat, hidden, classes):
    vmem = pl.BlockSpec(memory_space=pltpu.VMEM)
    shapes = [(feat, hidden), (feat, hidden), (1, hidden), (classes, hidden), (classes, hidden), (1, classes)]
    return pl.pallas_call(
        unpack_kernel,
        name="unpack",
        out_shape=tuple(jax.ShapeDtypeStruct(shape, jnp.float32) for shape in shapes),
        in_specs=[vmem],
        out_specs=(vmem,) * 6,
        compiler_params=pltpu.CompilerParams(vmem_limit_bytes=VMEM_LIMIT),
    )(packed)


def reduce_kernel(
    part_ref, out_ref, near_box, middle, far_box, gathered, send_sem, recv_sem, *, n_dom, n_rep, near,
):
    count = n_dom * n_rep
    far = count // near
    rows = part_ref.shape[0] // count
    span = far * rows
    me = lax.axis_index("dom") * n_rep + lax.axis_index("rep")
    here, there = lax.rem(me, near), me // near
    barrier = pltpu.get_barrier_semaphore()

    def place(index):
        return {"dom": index // n_rep, "rep": lax.rem(index, n_rep)}

    def near_peer(step):
        other = lax.rem(here + step, near)
        return other, place(there * near + other)

    def far_peer(step):
        other = lax.rem(there + step, far)
        return other, place(other * near + here)

    def wide_at(index):
        return pl.ds(pl.multiple_of(index * span, 8), span)

    def thin_at(index):
        return pl.ds(pl.multiple_of(index * rows, 8), rows)

    def greet_near(step, carry):
        pl.semaphore_signal(barrier, inc=1, device_id=near_peer(step)[1], device_id_type=MESH)
        return carry

    def greet_far(step, carry):
        pl.semaphore_signal(barrier, inc=1, device_id=far_peer(step)[1], device_id_type=MESH)
        return carry

    lax.fori_loop(1, near, greet_near, 0)
    lax.fori_loop(1, far, greet_far, 0)
    pl.semaphore_wait(barrier, near + far - 2)

    def copy(source, target, stage, where):
        return pltpu.make_async_remote_copy(
            source, target, send_sem.at[stage], recv_sem.at[stage], device_id=where, device_id_type=MESH
        )

    def out_near(step, carry):
        other, where = near_peer(step)
        copy(part_ref.at[wide_at(other)], near_box.at[wide_at(here)], 0, where).start()
        return carry

    lax.fori_loop(1, near, out_near, 0)
    some = pl.ds(0, (near - 1) * span)
    first = copy(part_ref.at[some], near_box.at[some], 0, near_peer(1)[1])
    first.wait_recv()

    def add_near(step, total):
        return total + near_box[wide_at(near_peer(step)[0]), :]

    middle[...] = lax.fori_loop(1, near, add_near, part_ref[wide_at(here), :])

    def out_far(step, carry):
        other, where = far_peer(step)
        copy(middle.at[thin_at(other)], far_box.at[thin_at(there)], 1, where).start()
        return carry

    lax.fori_loop(1, far, out_far, 0)
    some = pl.ds(0, (far - 1) * rows)
    second = copy(middle.at[some], far_box.at[some], 1, far_peer(1)[1])
    second.wait_recv()

    def add_far(step, total):
        return total + far_box[thin_at(far_peer(step)[0]), :]

    total = lax.fori_loop(1, far, add_far, middle[thin_at(there), :])
    mine = here * far + there
    gathered[mine] = total.astype(gathered.dtype)

    def back_far(step, carry):
        copy(gathered.at[mine], gathered.at[mine], 2, far_peer(step)[1]).start()
        return carry

    lax.fori_loop(1, far, back_far, 0)
    some = gathered.at[pl.ds(0, far - 1)]
    third = copy(some, some, 2, far_peer(1)[1])
    third.wait_recv()
    group = gathered.at[pl.ds(here * far, far)]

    def back_near(step, carry):
        copy(group, group, 3, near_peer(step)[1]).start()
        return carry

    lax.fori_loop(1, near, back_near, 0)
    some = gathered.at[pl.ds(0, (near - 1) * far)]
    fourth = copy(some, some, 3, near_peer(1)[1])
    fourth.wait_recv()
    first.wait_send()
    second.wait_send()
    third.wait_send()
    fourth.wait_send()
    for index in range(count):
        out_ref[index * rows : (index + 1) * rows, :] = gathered[index].astype(jnp.float32)


def sum_everywhere(pieces):
    n_dom, n_rep = lax.axis_size("dom"), lax.axis_size("rep")
    count = n_dom * n_rep
    near = 8
    far = count // near
    rows = pieces.shape[0] // count
    vmem = pl.BlockSpec(memory_space=pltpu.VMEM)
    return pl.pallas_call(
        functools.partial(reduce_kernel, n_dom=n_dom, n_rep=n_rep, near=near),
        name="sum_everywhere",
        out_shape=jax.ShapeDtypeStruct(pieces.shape, jnp.float32),
        in_specs=[vmem],
        out_specs=vmem,
        scratch_shapes=[
            pltpu.VMEM(pieces.shape, jnp.float32),
            pltpu.VMEM((far * rows, LANES), jnp.float32),
            pltpu.VMEM((far * rows, LANES), jnp.float32),
            pltpu.VMEM((count, rows, LANES), jnp.bfloat16),
            pltpu.SemaphoreType.DMA((4,)),
            pltpu.SemaphoreType.DMA((4,)),
        ],
        compiler_params=pltpu.CompilerParams(collective_id=1, has_side_effects=True, vmem_limit_bytes=VMEM_LIMIT),
    )(pieces)


def shards(
    features, partition_map, seed_ids, hop1_ids, hop2_ids, labels,
    self_one, neigh_one, bias_one, self_two, neigh_two, bias_two,
):
    parts = lax.axis_size("dom")
    count = parts * lax.axis_size("rep")
    seeds = seed_ids.shape[0]
    fan_one = hop1_ids.shape[1]
    fan_two = hop2_ids.shape[2]
    node_rows, feat = features.shape
    tree_rows = 1 + fan_one + fan_one * fan_two
    cold_cap = tree_rows // 2 * (seeds // parts)
    cap_row = round_up(cold_cap, 16)
    cap_pad = round_up(cold_cap, LANES)
    stride = HOT_DEV + cap_row
    total = seeds * tree_rows
    id_rows = total // LANES
    spare = round_up(id_rows, 8) * LANES - total
    wanted = [seed_ids, hop1_ids.reshape(-1), hop2_ids.reshape(-1), jnp.zeros((spare,), jnp.int32)]
    ids = jnp.concatenate(wanted).reshape(-1, LANES)
    request, addr = plan(ids, partition_map, parts, node_rows, stride, id_rows, cap_pad)
    table = exchange(request, features, cap_row, cap_pad // LANES).reshape(parts * stride, feat)
    hidden, classes = self_two.shape
    used = pack_plan(feat, hidden, classes)[-1]
    pack_rows = count * round_up(-(-used // count), 8)
    loss, pieces = model(
        addr.reshape(-1), table, labels, self_one, neigh_one, bias_one, self_two, neigh_two, bias_two,
        fan_one, fan_two, pack_rows,
    )
    grads = unpack(sum_everywhere(pieces), feat, hidden, classes)
    return (
        loss.reshape(-1), grads[0], grads[1], grads[2].reshape(-1),
        grads[3].T, grads[4].T, grads[5].reshape(-1),
    )


def solution(mesh):
    return jax.shard_map(
        shards,
        mesh=mesh,
        in_specs=(
            P("dom", None),
            P(),
            P(("dom", "rep")),
            P(("dom", "rep"), None),
            P(("dom", "rep"), None, None),
            P(("dom", "rep")),
            P(),
            P(),
            P(),
            P(),
            P(),
            P(),
        ),
        out_specs=(P(("dom", "rep")), P(), P(), P(), P(), P(), P()),
        check_vma=False,
    )
```

```python
import functools

import jax
import jax.numpy as jnp
from jax import lax
from jax.experimental import pallas as pl
from jax.experimental.pallas import tpu as pltpu
from jax.sharding import PartitionSpec as P

HOT_DEV = 256
LANES = 128
MESH = pl.DeviceIdType.MESH
VMEM_LIMIT = 56 * 1024 * 1024


def round_up(value, unit):
    return -(-value // unit) * unit


def dot_tn(left, right):
    return lax.dot_general(left, right, (((0,), (0,)), ((), ())), preferred_element_type=jnp.float32)


def dot_nt(left, right):
    return lax.dot_general(left, right, (((1,), (1,)), ((), ())), preferred_element_type=jnp.float32)


def dot_nn(left, right):
    return jnp.dot(left, right, preferred_element_type=jnp.float32)


def plan_kernel(ids_ref, map_ref, req_ref, addr_ref, own_ref, slot_ref, val_ref, pos_ref, pieces_ref, *, parts, shift, stride, id_rows, cap_pad):
    rows = ids_ref.shape[0]
    blocks = rows // 8
    stored = map_ref[...]
    pieces = jnp.concatenate([stored >> 16, (stored >> 8) & 255, stored & 255], axis=1)
    pieces_ref[...] = pieces.astype(jnp.float32).T.astype(jnp.bfloat16)
    map_iota = lax.broadcasted_iota(jnp.int32, map_ref.shape, 0)
    lane_iota = lax.broadcasted_iota(jnp.int32, (LANES, 2 * LANES), 0)

    def lookup(step, carry):
        base = pl.multiple_of(step * 8, 8)
        tile = ids_ref[pl.ds(base, 8), :]
        high, low = tile >> 7, tile & (LANES - 1)
        for k in range(0, 8, 2):
            hot = [(map_iota == high[q : q + 1, :]).astype(jnp.bfloat16) for q in (k, k + 1)]
            found = dot_nn(pieces_ref[...], jnp.concatenate(hot, axis=1))
            found = found[:LANES] * 65536.0 + found[LANES : 2 * LANES] * 256.0 + found[2 * LANES :]
            lane = jnp.concatenate([low[k : k + 1, :], low[k + 1 : k + 2, :]], axis=1)
            picked = jnp.sum(jnp.where(lane_iota == lane, found, 0.0), axis=0, keepdims=True)
            pos_ref[pl.ds(base + k, 1), :] = picked[:, :LANES].astype(jnp.int32)
            pos_ref[pl.ds(base + k + 1, 1), :] = picked[:, LANES:].astype(jnp.int32)
        return carry

    lax.fori_loop(0, blocks, lookup, 0)
    position = pos_ref[...]
    owner = position >> shift
    local = position & ((1 << shift) - 1)
    row_iota = lax.broadcasted_iota(jnp.int32, (rows, LANES), 0)
    is_cold = (local >= HOT_DEV) & (row_iota < id_rows)
    owner_cold = jnp.where(is_cold, owner, -1)
    upper = (
        lax.broadcasted_iota(jnp.int32, (LANES, LANES), 0) <= lax.broadcasted_iota(jnp.int32, (LANES, LANES), 1)
    ).astype(jnp.bfloat16)
    ones = jnp.ones((LANES, LANES), jnp.bfloat16)
    below = (
        lax.broadcasted_iota(jnp.int32, (rows, rows), 1) < lax.broadcasted_iota(jnp.int32, (rows, rows), 0)
    ).astype(jnp.bfloat16)
    slot = jnp.full((rows, LANES), -1.0, jnp.float32)
    for part in range(parts):
        hit = owner_cold == part
        member = hit.astype(jnp.bfloat16)
        ahead = dot_nn(below, member).astype(jnp.bfloat16)
        running = dot_nn(member, upper) + dot_nn(ahead, ones)
        slot = jnp.where(hit, running - 1.0, slot)
    slot = slot.astype(jnp.int32)
    addr_ref[...] = owner * stride + jnp.where(is_cold, HOT_DEV + slot, local)
    own_ref[...] = owner_cold
    slot_ref[...] = slot
    val_ref[...] = local
    part_iota = lax.broadcasted_iota(jnp.int32, (parts, LANES), 0)
    slot_iota = lax.broadcasted_iota(jnp.int32, (cap_pad, LANES), 0)

    def place(step, table):
        base = pl.multiple_of(step * 8, 8)
        own8 = own_ref[pl.ds(base, 8), :]
        slot8 = slot_ref[pl.ds(base, 8), :]
        val8 = val_ref[pl.ds(base, 8), :]
        for k in range(0, 8, 2):
            lefts, rights = [], []
            for q in range(k, k + 2):
                val = val8[q : q + 1, :].astype(jnp.float32)
                top = jnp.floor(val * (1.0 / LANES))
                mine = part_iota == own8[q : q + 1, :]
                lefts.append(
                    jnp.concatenate(
                        [jnp.where(mine, top, 0.0), jnp.where(mine, val - top * LANES, 0.0)], axis=0
                    ).astype(jnp.bfloat16)
                )
                rights.append((slot_iota == slot8[q : q + 1, :]).astype(jnp.bfloat16))
            table = table + dot_nt(jnp.concatenate(lefts, axis=1), jnp.concatenate(rights, axis=1))
        return table

    table = lax.fori_loop(0, blocks, place, jnp.zeros((2 * parts, cap_pad), jnp.float32))
    request = (table[:parts] * LANES + table[parts:]).astype(jnp.int32)
    req_ref[...] = jnp.zeros(req_ref.shape, jnp.int32)
    for c in range(cap_pad // LANES):
        req_ref[:, c, :] = request[:, c * LANES : (c + 1) * LANES]


def plan(ids, partition_map, parts, node_rows, stride, id_rows, cap_pad):
    rows = ids.shape[0]
    kernel = functools.partial(
        plan_kernel,
        parts=parts,
        shift=node_rows.bit_length() - 1,
        stride=stride,
        id_rows=id_rows,
        cap_pad=cap_pad,
    )
    return pl.pallas_call(
        kernel,
        name="plan",
        out_shape=(
            jax.ShapeDtypeStruct((parts, round_up(cap_pad // LANES, 8), LANES), jnp.int32),
            jax.ShapeDtypeStruct((rows, LANES), jnp.int32),
        ),
        in_specs=[pl.BlockSpec(memory_space=pltpu.VMEM)] * 2,
        out_specs=(pl.BlockSpec(memory_space=pltpu.VMEM),) * 2,
        scratch_shapes=[pltpu.VMEM((rows, LANES), jnp.int32)] * 4
        + [pltpu.VMEM((3 * LANES, partition_map.size // LANES), jnp.bfloat16)],
        compiler_params=pltpu.CompilerParams(vmem_limit_bytes=VMEM_LIMIT),
        cost_estimate=pl.CostEstimate(flops=40_000_000, bytes_accessed=1_000_000, transcendentals=0),
    )(ids, partition_map.reshape(-1, LANES))


ROOT = 0.7978845608028654
CUBE = 0.044715


def gelu_pair(pre):
    square = pre * pre
    bend = jnp.tanh(ROOT * pre * (1.0 + CUBE * square))
    half = 0.5 * (1.0 + bend)
    slope = half + 0.5 * pre * (1.0 - bend * bend) * (ROOT * (1.0 + 3.0 * CUBE * square))
    return pre * half, slope


def tree_sum(values):
    while len(values) > 1:
        values = [a + b for a, b in zip(values[::2], values[1::2])] + (
            [values[-1]] if len(values) % 2 else []
        )
    return values[0]


def model_kernel(
    addr_ref, table_ref, label_ref, self_one, neigh_one, b_one_ref, self_two, neigh_two, b_two_ref,
    loss_ref, pack_ref,
    wide, x_buf, far_buf, own_buf, slope_buf, d_buf, *, seeds, fan_one, fan_two,
):
    feat = table_ref.shape[1]
    hidden = self_one.shape[1]
    hops = seeds * fan_one
    chunk = 64 if table_ref.shape[0] % 64 == 0 else 16

    def widen(step, carry):
        at = pl.ds(pl.multiple_of(step * chunk, chunk), chunk)
        wide[at, :] = table_ref[at, :].astype(jnp.float32)
        return carry

    lax.fori_loop(0, table_ref.shape[0] // chunk, widen, 0)

    def fetch(step, carry):
        j = step // (seeds // 8)
        block = step % (seeds // 8)
        base = pl.multiple_of(step * 8, 8)
        for k in range(8):
            hop = (block * 8 + k) * fan_one + j
            own_buf[pl.ds(base + k, 1), :] = wide[pl.ds(addr_ref[seeds + hop], 1), :]
            first = seeds + hops + hop * fan_two
            rows = [wide[pl.ds(addr_ref[first + m], 1), :] for m in range(fan_two)]
            far_buf[pl.ds(base + k, 1), :] = tree_sum(rows)
        return carry

    lax.fori_loop(0, hops // 8, fetch, 0)

    def fetch_seed(step, carry):
        base = pl.multiple_of(step * 8, 8)
        for k in range(8):
            own_buf[pl.ds(hops + base + k, 1), :] = wide[pl.ds(addr_ref[base + k], 1), :]
        return carry

    lax.fori_loop(0, seeds // 8, fetch_seed, 0)

    w_one = jnp.concatenate([self_one[...], neigh_one[...]], axis=0)
    w_two = jnp.concatenate([self_two[...], neigh_two[...]], axis=1)
    b_one = b_one_ref[...]
    row_sum = jnp.zeros((seeds, feat), jnp.float32)
    hid_sum = jnp.zeros((seeds, hidden), jnp.float32)
    for j in range(fan_one):
        at = slice(j * seeds, (j + 1) * seeds)
        own = own_buf[at, :]
        row_sum = row_sum + own
        x_buf[at, :feat] = own.astype(jnp.bfloat16)
        x_buf[at, feat:] = (far_buf[at, :] * (1.0 / fan_two)).astype(jnp.bfloat16)
    x_buf[hops:, :feat] = own_buf[hops:, :].astype(jnp.bfloat16)
    x_buf[hops:, feat:] = (row_sum * (1.0 / fan_one)).astype(jnp.bfloat16)
    act = None
    for j in range(fan_one + 1):
        at = slice(j * seeds, (j + 1) * seeds)
        act, slope = gelu_pair(dot_nn(x_buf[at, :], w_one) + b_one)
        act = act.astype(jnp.bfloat16)
        slope_buf[at, :] = slope
        if j < fan_one:
            hid_sum = hid_sum + act.astype(jnp.float32)
    hid = jnp.concatenate([act, (hid_sum * (1.0 / fan_one)).astype(jnp.bfloat16)], axis=1)
    logits = dot_nt(hid, w_two) + b_two_ref[...]
    shifted = logits - jnp.max(logits, axis=1, keepdims=True)
    log_probs = shifted - jnp.log(jnp.sum(jnp.exp(shifted), axis=1, keepdims=True))
    class_iota = lax.broadcasted_iota(jnp.int32, logits.shape, 1)
    diagonal = lax.broadcasted_iota(jnp.int32, (seeds, seeds), 0) == lax.broadcasted_iota(jnp.int32, (seeds, seeds), 1)
    label = jnp.sum(jnp.where(diagonal, label_ref[...].astype(jnp.float32), 0.0), axis=1, keepdims=True)
    target = (class_iota.astype(jnp.float32) == label).astype(jnp.float32)
    loss = jnp.sum(log_probs * target, axis=1, keepdims=True)
    loss_ref[...] = -jnp.sum(jnp.where(diagonal, loss, 0.0), axis=0, keepdims=True)
    d_logits = ((jnp.exp(log_probs) - target) * (1.0 / seeds)).astype(jnp.bfloat16)
    g_two = dot_tn(d_logits, hid)
    gb_two = jnp.sum(d_logits.astype(jnp.float32), axis=0, keepdims=True)
    d_hid = dot_nn(d_logits, w_two)
    d_hop = d_hid[:, hidden:] * (1.0 / fan_one)
    for j in range(fan_one + 1):
        at = slice(j * seeds, (j + 1) * seeds)
        d_pre = ((d_hop if j < fan_one else d_hid[:, :hidden]) * slope_buf[at, :]).astype(jnp.bfloat16)
        d_buf[at, :] = d_pre
    gb_one = dot_nn(jnp.ones((8, d_buf.shape[0]), jnp.bfloat16), d_buf[...])[:1]
    pack_gradients(pack_ref, dot_tn(x_buf[...], d_buf[...]), gb_one, g_two, gb_two)


def model(addr, table, labels, self_one, neigh_one, bias_one, self_two, neigh_two, bias_two, fan_one, fan_two, pack_rows):
    seeds = labels.shape[0]
    feat, hidden = self_one.shape
    classes = self_two.shape[1]
    total = seeds * (1 + fan_one)
    vmem = pl.BlockSpec(memory_space=pltpu.VMEM)
    return pl.pallas_call(
        functools.partial(model_kernel, seeds=seeds, fan_one=fan_one, fan_two=fan_two),
        name="model",
        out_shape=(
            jax.ShapeDtypeStruct((1, seeds), jnp.float32),
            jax.ShapeDtypeStruct((pack_rows, LANES), jnp.float32),
        ),
        in_specs=[pl.BlockSpec(memory_space=pltpu.SMEM)] + [vmem] * 8,
        out_specs=(vmem,) * 2,
        scratch_shapes=[
            pltpu.VMEM(table.shape, jnp.float32),
            pltpu.VMEM((total, 2 * feat), jnp.bfloat16),
            pltpu.VMEM((total - seeds, feat), jnp.float32),
            pltpu.VMEM((total, feat), jnp.float32),
            pltpu.VMEM((total, hidden), jnp.float32),
            pltpu.VMEM((total, hidden), jnp.bfloat16),
        ],
        compiler_params=pltpu.CompilerParams(vmem_limit_bytes=VMEM_LIMIT),
        cost_estimate=pl.CostEstimate(flops=100_000_000, bytes_accessed=4_000_000, transcendentals=0),
    )(
        addr,
        table,
        labels.reshape(1, seeds),
        self_one,
        neigh_one,
        bias_one.reshape(1, hidden),
        self_two.T,
        neigh_two.T,
        bias_two.reshape(1, classes),
    )


def exchange_kernel(
    req_ref, feat_ref, out_ref, inbox, wanted, wide, stage, send,
    local_sem, req_send, req_recv, hub_send, hub_recv, row_send, row_recv, *, parts, asks,
):
    node_rows = feat_ref.shape[0]
    cap_row = send.shape[1]
    me = lax.axis_index("dom")
    bits = parts.bit_length() - 1
    barrier = pltpu.get_barrier_semaphore()

    def partner(mask):
        other = me ^ mask
        return other, {"dom": other}

    def greet(step, carry):
        pl.semaphore_signal(barrier, inc=1, device_id=partner(step)[1], device_id_type=MESH)
        return carry

    lax.fori_loop(1, parts, greet, 0)
    hub_at = pl.ds(0, HOT_DEV)
    ask_at = pl.ds(0, asks)
    keep_req = pltpu.make_async_copy(req_ref.at[me], inbox.at[me], local_sem.at[0])
    keep_req.start()
    keep_hub = pltpu.make_async_copy(feat_ref.at[hub_at], out_ref.at[me, hub_at], local_sem.at[1])
    keep_hub.start()
    pl.semaphore_wait(barrier, parts - 1)

    def ask(step, carry):
        other, at = partner(parts - step)
        pltpu.make_async_remote_copy(
            req_ref.at[other, ask_at], inbox.at[me, ask_at], req_send, req_recv, device_id=at, device_id_type=MESH
        ).start()
        return carry

    lax.fori_loop(1, parts, ask, 0)
    keep_hub.wait()

    def held(level, index):
        return me ^ (index * (parts >> level))

    def share(level):
        at = partner(parts >> (level + 1))[1]

        def one(index, carry):
            slot = held(level, index)
            pltpu.make_async_remote_copy(
                out_ref.at[slot, hub_at], out_ref.at[slot, hub_at], hub_send.at[level], hub_recv.at[level],
                device_id=at, device_id_type=MESH,
            ).start()
            return carry

        lax.fori_loop(0, 1 << level, one, 0)

    def shared(level):
        some = out_ref.at[pl.ds(0, 1 << level), hub_at]
        return pltpu.make_async_remote_copy(
            some, some, hub_send.at[level], hub_recv.at[level], device_id=partner(1)[1], device_id_type=MESH
        )

    share(0)

    def widen(step, carry):
        at = pl.ds(pl.multiple_of(step * 64, 64), 64)
        wide[at, :] = feat_ref[at, :].astype(jnp.float32)
        return carry

    lax.fori_loop(0, node_rows // 64, widen, 0)
    most = pl.ds(0, parts - 1)
    asked = pltpu.make_async_remote_copy(
        req_ref.at[most, ask_at], inbox.at[most, ask_at], req_send, req_recv,
        device_id=partner(1)[1], device_id_type=MESH,
    )
    keep_req.wait()
    asked.wait_recv()
    to_scalar = pltpu.make_async_copy(inbox.at[:, ask_at], wanted, local_sem.at[2])
    to_scalar.start()
    to_scalar.wait()

    def collect(other):
        def block(step, carry):
            base = pl.multiple_of(step * 16, 16)
            row = step // (LANES // 16)
            lane = lax.rem(step, LANES // 16) * 16
            for k in range(16):
                stage[pl.ds(base + k, 1), :] = wide[pl.ds(wanted[other, row, lane + k], 1), :]
            return carry

        lax.fori_loop(0, cap_row // 16, block, 0)
        return stage[...].astype(jnp.bfloat16)

    rows_at = pl.ds(HOT_DEV, cap_row)

    def serve(step, carry):
        other, at = partner(parts - step)
        send[other] = collect(other)
        pltpu.make_async_remote_copy(
            send.at[other], out_ref.at[me, rows_at], row_send, row_recv, device_id=at, device_id_type=MESH
        ).start()
        return carry

    served = 1
    for level in range(1, bits):
        until = max(1, parts * (level - 1) // bits)
        lax.fori_loop(served, until, serve, 0)
        served = until
        shared(level - 1).wait_recv()
        share(level)
    lax.fori_loop(served, parts, serve, 0)
    out_ref[me, HOT_DEV:, :] = collect(me)
    rows = pltpu.make_async_remote_copy(
        send.at[most], out_ref.at[most, rows_at], row_send, row_recv, device_id=partner(1)[1], device_id_type=MESH
    )
    asked.wait_send()
    shared(bits - 1).wait_recv()
    for level in range(bits):
        shared(level).wait_send()
    rows.wait()


def exchange(request, features, cap_row, asks):
    parts = lax.axis_size("dom")
    bits = parts.bit_length() - 1
    node_rows, feat = features.shape
    vmem = pl.BlockSpec(memory_space=pltpu.VMEM)
    return pl.pallas_call(
        functools.partial(exchange_kernel, parts=parts, asks=asks),
        name="exchange",
        out_shape=jax.ShapeDtypeStruct((parts, HOT_DEV + cap_row, feat), features.dtype),
        in_specs=[vmem, vmem],
        out_specs=vmem,
        scratch_shapes=[
            pltpu.VMEM(request.shape, jnp.int32),
            pltpu.SMEM((parts, asks, LANES), jnp.int32),
            pltpu.VMEM((node_rows, feat), jnp.float32),
            pltpu.VMEM((cap_row, feat), jnp.float32),
            pltpu.VMEM((parts, cap_row, feat), features.dtype),
            pltpu.SemaphoreType.DMA((3,)),
            pltpu.SemaphoreType.DMA,
            pltpu.SemaphoreType.DMA,
            pltpu.SemaphoreType.DMA((bits,)),
            pltpu.SemaphoreType.DMA((bits,)),
            pltpu.SemaphoreType.DMA,
            pltpu.SemaphoreType.DMA,
        ],
        compiler_params=pltpu.CompilerParams(collective_id=2, has_side_effects=True, vmem_limit_bytes=VMEM_LIMIT),
    )(request, features)


def pack_plan(feat, hidden, classes):
    halves = hidden // LANES
    one = 2 * feat * halves
    high = round_up(classes, 8)
    tail = one + 2 * halves * high
    return halves, one, high, tail, tail + 8


def pack_gradients(pack_ref, g_one, gb_one, g_two, gb_two):
    hidden, feat = g_one.shape[1], g_one.shape[0] // 2
    classes = g_two.shape[0]
    halves, one, high, tail, used = pack_plan(feat, hidden, classes)
    for h in range(halves):
        pack_ref[h * 2 * feat : (h + 1) * 2 * feat, :] = g_one[:, h * LANES : (h + 1) * LANES]
    pack_ref[one:, :] = jnp.zeros((pack_ref.shape[0] - one, LANES), jnp.float32)
    for h in range(2 * halves):
        pack_ref[one + h * high : one + h * high + classes, :] = g_two[:, h * LANES : (h + 1) * LANES]
    for h in range(halves):
        pack_ref[tail + h : tail + h + 1, :] = gb_one[:, h * LANES : (h + 1) * LANES]
    pack_ref[tail + halves : tail + halves + 1, :] = gb_two[:, :LANES]
    pack_ref[tail + halves + 1 : tail + halves + 2, : classes - LANES] = gb_two[:, LANES:]


def unpack_kernel(pack_ref, self_one, neigh_one, bias_one, self_two, neigh_two, bias_two):
    feat, hidden = self_one.shape
    classes = self_two.shape[0]
    halves, one, high, tail, used = pack_plan(feat, hidden, classes)
    for h in range(halves):
        cols = slice(h * LANES, (h + 1) * LANES)
        at = h * 2 * feat
        self_one[:, cols] = pack_ref[at : at + feat, :]
        neigh_one[:, cols] = pack_ref[at + feat : at + 2 * feat, :]
        at = one + h * high
        self_two[:, cols] = pack_ref[at : at + classes, :]
        at = one + (halves + h) * high
        neigh_two[:, cols] = pack_ref[at : at + classes, :]
        bias_one[:, cols] = pack_ref[tail + h : tail + h + 1, :]
    bias_two[:, :LANES] = pack_ref[tail + halves : tail + halves + 1, :]
    bias_two[:, LANES:] = pack_ref[tail + halves + 1 : tail + halves + 2, : classes - LANES]


def unpack(packed, feat, hidden, classes):
    vmem = pl.BlockSpec(memory_space=pltpu.VMEM)
    shapes = [(feat, hidden), (feat, hidden), (1, hidden), (classes, hidden), (classes, hidden), (1, classes)]
    return pl.pallas_call(
        unpack_kernel,
        name="unpack",
        out_shape=tuple(jax.ShapeDtypeStruct(shape, jnp.float32) for shape in shapes),
        in_specs=[vmem],
        out_specs=(vmem,) * 6,
        compiler_params=pltpu.CompilerParams(vmem_limit_bytes=VMEM_LIMIT),
    )(packed)


def reduce_kernel(
    part_ref, out_ref, near_box, middle, far_box, gathered, send_sem, recv_sem, *, n_dom, n_rep, near,
):
    count = n_dom * n_rep
    far = count // near
    rows = part_ref.shape[0] // count
    span = far * rows
    me = lax.axis_index("dom") * n_rep + lax.axis_index("rep")
    here, there = lax.rem(me, near), me // near
    barrier = pltpu.get_barrier_semaphore()

    def place(index):
        return {"dom": index // n_rep, "rep": lax.rem(index, n_rep)}

    def near_peer(step):
        other = lax.rem(here + step, near)
        return other, place(there * near + other)

    def far_peer(step):
        other = lax.rem(there + step, far)
        return other, place(other * near + here)

    def wide_at(index):
        return pl.ds(pl.multiple_of(index * span, 8), span)

    def thin_at(index):
        return pl.ds(pl.multiple_of(index * rows, 8), rows)

    def greet_near(step, carry):
        pl.semaphore_signal(barrier, inc=1, device_id=near_peer(step)[1], device_id_type=MESH)
        return carry

    def greet_far(step, carry):
        pl.semaphore_signal(barrier, inc=1, device_id=far_peer(step)[1], device_id_type=MESH)
        return carry

    lax.fori_loop(1, near, greet_near, 0)
    lax.fori_loop(1, far, greet_far, 0)
    pl.semaphore_wait(barrier, near + far - 2)

    def copy(source, target, stage, where):
        return pltpu.make_async_remote_copy(
            source, target, send_sem.at[stage], recv_sem.at[stage], device_id=where, device_id_type=MESH
        )

    def out_near(step, carry):
        other, where = near_peer(step)
        copy(part_ref.at[wide_at(other)], near_box.at[wide_at(here)], 0, where).start()
        return carry

    lax.fori_loop(1, near, out_near, 0)
    some = pl.ds(0, (near - 1) * span)
    first = copy(part_ref.at[some], near_box.at[some], 0, near_peer(1)[1])
    first.wait_recv()

    def add_near(step, total):
        return total + near_box[wide_at(near_peer(step)[0]), :]

    middle[...] = lax.fori_loop(1, near, add_near, part_ref[wide_at(here), :])

    def out_far(step, carry):
        other, where = far_peer(step)
        copy(middle.at[thin_at(other)], far_box.at[thin_at(there)], 1, where).start()
        return carry

    lax.fori_loop(1, far, out_far, 0)
    some = pl.ds(0, (far - 1) * rows)
    second = copy(middle.at[some], far_box.at[some], 1, far_peer(1)[1])
    second.wait_recv()

    def add_far(step, total):
        return total + far_box[thin_at(far_peer(step)[0]), :]

    total = lax.fori_loop(1, far, add_far, middle[thin_at(there), :])
    mine = here * far + there
    gathered[mine] = total.astype(gathered.dtype)

    def back_far(step, carry):
        copy(gathered.at[mine], gathered.at[mine], 2, far_peer(step)[1]).start()
        return carry

    lax.fori_loop(1, far, back_far, 0)
    some = gathered.at[pl.ds(0, far - 1)]
    third = copy(some, some, 2, far_peer(1)[1])
    third.wait_recv()
    group = gathered.at[pl.ds(here * far, far)]

    def back_near(step, carry):
        copy(group, group, 3, near_peer(step)[1]).start()
        return carry

    lax.fori_loop(1, near, back_near, 0)
    some = gathered.at[pl.ds(0, (near - 1) * far)]
    fourth = copy(some, some, 3, near_peer(1)[1])
    fourth.wait_recv()
    first.wait_send()
    second.wait_send()
    third.wait_send()
    fourth.wait_send()
    for index in range(count):
        out_ref[index * rows : (index + 1) * rows, :] = gathered[index].astype(jnp.float32)


def sum_everywhere(pieces):
    n_dom, n_rep = lax.axis_size("dom"), lax.axis_size("rep")
    count = n_dom * n_rep
    near = 8
    far = count // near
    rows = pieces.shape[0] // count
    vmem = pl.BlockSpec(memory_space=pltpu.VMEM)
    return pl.pallas_call(
        functools.partial(reduce_kernel, n_dom=n_dom, n_rep=n_rep, near=near),
        name="sum_everywhere",
        out_shape=jax.ShapeDtypeStruct(pieces.shape, jnp.float32),
        in_specs=[vmem],
        out_specs=vmem,
        scratch_shapes=[
            pltpu.VMEM(pieces.shape, jnp.float32),
            pltpu.VMEM((far * rows, LANES), jnp.float32),
            pltpu.VMEM((far * rows, LANES), jnp.float32),
            pltpu.VMEM((count, rows, LANES), jnp.bfloat16),
            pltpu.SemaphoreType.DMA((4,)),
            pltpu.SemaphoreType.DMA((4,)),
        ],
        compiler_params=pltpu.CompilerParams(collective_id=1, has_side_effects=True, vmem_limit_bytes=VMEM_LIMIT),
    )(pieces)


def shards(
    features, partition_map, seed_ids, hop1_ids, hop2_ids, labels,
    self_one, neigh_one, bias_one, self_two, neigh_two, bias_two,
):
    parts = lax.axis_size("dom")
    count = parts * lax.axis_size("rep")
    seeds = seed_ids.shape[0]
    fan_one = hop1_ids.shape[1]
    fan_two = hop2_ids.shape[2]
    node_rows, feat = features.shape
    tree_rows = 1 + fan_one + fan_one * fan_two
    cold_cap = tree_rows // 2 * (seeds // parts)
    cap_row = round_up(cold_cap, 16)
    cap_pad = round_up(cold_cap, LANES)
    stride = HOT_DEV + cap_row
    total = seeds * tree_rows
    id_rows = total // LANES
    spare = round_up(id_rows, 8) * LANES - total
    wanted = [seed_ids, hop1_ids.reshape(-1), hop2_ids.reshape(-1), jnp.zeros((spare,), jnp.int32)]
    ids = jnp.concatenate(wanted).reshape(-1, LANES)
    request, addr = plan(ids, partition_map, parts, node_rows, stride, id_rows, cap_pad)
    table = exchange(request, features, cap_row, cap_pad // LANES).reshape(parts * stride, feat)
    hidden, classes = self_two.shape
    used = pack_plan(feat, hidden, classes)[-1]
    pack_rows = count * round_up(-(-used // count), 8)
    loss, pieces = model(
        addr.reshape(-1), table, labels, self_one, neigh_one, bias_one, self_two, neigh_two, bias_two,
        fan_one, fan_two, pack_rows,
    )
    grads = unpack(sum_everywhere(pieces), feat, hidden, classes)
    return (
        loss.reshape(-1), grads[0], grads[1], grads[2].reshape(-1),
        grads[3].T, grads[4].T, grads[5].reshape(-1),
    )


def solution(mesh):
    return jax.shard_map(
        shards,
        mesh=mesh,
        in_specs=(
            P("dom", None),
            P(),
            P(("dom", "rep")),
            P(("dom", "rep"), None),
            P(("dom", "rep"), None, None),
            P(("dom", "rep")),
            P(),
            P(),
            P(),
            P(),
            P(),
            P(),
        ),
        out_specs=(P(("dom", "rep")), P(), P(), P(), P(), P(), P()),
        check_vma=False,
    )
```
